32 devices in a mesh: outer: 4 (over y, core), inner: 8 (over z, x).
Axes of the slice: x: 2, y: 2, z: 4, core: 2. Of those that a mesh axis runs over, the one named last changes fastest.
Arguments:
- points: float32 [65536, 64], P(('outer', 'inner')), may hold values from -2.5 to 2.5
- charges: float32 [65536, 128], P(('outer', 'inner')), may hold values from -0.4 to 0.4
- interp: float32 [65536, 256], P(('outer', 'inner')), may hold values from -0.25 to 0.25
- order: int32 [65536], P(('outer', 'inner')), may hold values from 0 to 65535, as said below
- near: int32 [128, 8], replicated, may hold values from 0 to 127, as said below
- far: int32 [128, 8], replicated, may hold values from 0 to 127, as said below
- skel: int32 [128, 256], P(('outer', 'inner')), may hold values from 0 to 511, as said below
Outputs:
- potential: float32 [65536, 128], P(('outer', 'inner'))
The draws below stay inside these ranges and needn't reach their ends.
Inputs may be any that keep to these rules, and one draw needn't show every extreme that they name: `order`: A permutation; tree position p lies on device p // 2048 in the rows' layout, and each device's rows hold exactly 64 positions of every device. `near`: row g names leaf g first, then 8 - 1 distinct leaves on other devices with the same outer index (leaf h lies on device h // 4); the entries of one device's leaves name at most 4 leaves on any one other device, counting repeats, and some pair of devices reaches 4. `far`: row g names 8 distinct leaves on devices with the same inner index as leaf g and another outer index. `skel`: each row holds distinct values.
All inputs are finite; a program needn't handle non-finite values.
Results may differ from the reference program's by a relative error of at most 0.000082.
Values sent between devices are 32-bit elements; how exact they have to be, the bound alone decides.
No kernel may reach another device: no remote copies, remote signals or barrier semaphores. Data moves between devices by JAX's collectives and lax.ppermute only.
A program may use at most 128 MiB of HBM per device.

```python
import jax
import jax.numpy as jnp
from jax import lax

DIM = 64
RHS = 128
LEAF = 512
SKEL = 256
NEAR = 8
FARS = 8
LEAF_DEV = 4
POINTS = 65536
N_OUTER = 4
N_INNER = 8


def order_table(key):
    device_total = N_OUTER * N_INNER
    row_total = LEAF_DEV * LEAF
    per_device = row_total // device_total
    halves = jax.random.split(jax.random.fold_in(key, 11), 2)
    dest_perm = jax.vmap(lambda sub: jax.random.permutation(sub, row_total))(jax.random.split(halves[0], device_total))
    src_perm = jax.vmap(lambda sub: jax.random.permutation(sub, row_total))(jax.random.split(halves[1], device_total))
    tree_pos = jnp.arange(device_total, dtype=jnp.int32)[None, :, None] * row_total + jnp.transpose(dest_perm.reshape(device_total, device_total, per_device), (1, 0, 2)).astype(jnp.int32)
    orig_pos = jnp.arange(device_total, dtype=jnp.int32)[:, None, None] * row_total + src_perm.reshape(device_total, device_total, per_device).astype(jnp.int32)
    table = jnp.zeros((device_total * row_total,), jnp.int32)
    return table.at[orig_pos.reshape(-1)].set(tree_pos.reshape(-1))


def draw_order(key, part):
    return order_table(key)


def draw_points(key, part):
    placed = order_table(key)
    leaf_total = N_OUTER * N_INNER * LEAF_DEV
    centers = jnp.clip(0.25 * jax.random.normal(jax.random.fold_in(key, 12), (leaf_total, DIM), jnp.float32), -1.0, 1.0)
    noise = jnp.clip(0.3 * jax.random.normal(jax.random.fold_in(key, 13), (leaf_total * LEAF, DIM), jnp.float32), -1.5, 1.5)
    tree_ordered_points = jnp.repeat(centers, LEAF, axis=0) + noise
    return tree_ordered_points[placed]


def draw_near(key, part):
    device_total = N_OUTER * N_INNER
    remote = NEAR - 1
    entries = LEAF_DEV * remote
    peer_total = N_INNER - 1
    capacity = (entries + N_INNER - 2) // (N_INNER - 1)

    def one_device(dev_key, device):
        first_key, second_key = jax.random.split(dev_key)
        local_pick = jax.vmap(lambda sub: jax.random.permutation(sub, LEAF_DEV)[:capacity])(jax.random.split(first_key, peer_total))
        chosen = jax.random.permutation(second_key, peer_total * capacity)[:entries]
        peer_slot = chosen // capacity
        local_leaf = local_pick.reshape(-1)[chosen]
        outer_pos = device // N_INNER
        inner_pos = device % N_INNER
        peer_inner = (inner_pos + 1 + peer_slot) % N_INNER
        listed = (outer_pos * N_INNER + peer_inner) * LEAF_DEV + local_leaf
        own_leaf = device * LEAF_DEV + jnp.arange(LEAF_DEV, dtype=jnp.int32)
        return jnp.concatenate([own_leaf[:, None], listed.reshape(LEAF_DEV, remote).astype(jnp.int32)], axis=1)
    tables = jax.vmap(one_device)(jax.random.split(jax.random.fold_in(key, 21), device_total), jnp.arange(device_total, dtype=jnp.int32))
    return tables.reshape(device_total * LEAF_DEV, NEAR).astype(jnp.int32)


def draw_far(key, part):
    leaf_total = N_OUTER * N_INNER * LEAF_DEV
    candidates = (N_OUTER - 1) * LEAF_DEV

    def one_leaf(leaf_key, leaf_id):
        picked = jax.random.permutation(leaf_key, candidates)[:FARS]
        device = leaf_id // LEAF_DEV
        outer_pos = device // N_INNER
        inner_pos = device % N_INNER
        other_outer = (outer_pos + 1 + picked // LEAF_DEV) % N_OUTER
        return ((other_outer * N_INNER + inner_pos) * LEAF_DEV + picked % LEAF_DEV).astype(jnp.int32)
    return jax.vmap(one_leaf)(jax.random.split(jax.random.fold_in(key, 31), leaf_total), jnp.arange(leaf_total, dtype=jnp.int32))


def draw_skel(key, part):
    leaf_total = N_OUTER * N_INNER * LEAF_DEV
    picks = jax.vmap(lambda sub: jax.random.permutation(sub, LEAF)[:SKEL])(jax.random.split(jax.random.fold_in(key, 41), leaf_total))
    return picks.astype(jnp.int32)


def levels(own_key, extent, cuts, least, largest):
    level, own = 1.0, jax.random.fold_in(own_key, 6)
    for dim, parts in cuts:
        draws = jnp.exp(jax.random.uniform(jax.random.fold_in(own, dim), (parts,), jnp.float32, least / len(cuts), largest / len(cuts)))
        level = level * jnp.repeat(draws, extent[dim] // parts).reshape([-1 if axis == dim else 1 for axis in range(len(extent))])
    return level


def bell_draw(stream_key, dims, deviation, limit, shards=(), held_as=jnp.bfloat16):
    values = deviation * jax.random.normal(stream_key, dims, jnp.float32)
    if shards:
        values = values * levels(stream_key, dims, shards, -0.22, 0.18)
    return jnp.clip(values, -limit, limit).astype(held_as)


def setup_inputs(seed: int = 0) -> dict:
    splits = jax.random.split(jax.random.key(seed), 8)
    return {
        "points": draw_points(jax.random.fold_in(splits[7], 71), 0),
        "charges": bell_draw(splits[1], (POINTS, RHS), 0.05, 0.4, ((0, 32),), jnp.float32),
        "interp": bell_draw(splits[2], (POINTS, SKEL), LEAF ** -0.5, 0.25, ((0, 32),), jnp.float32),
        "order": draw_order(jax.random.fold_in(splits[7], 71), 0),
        "near": draw_near(jax.random.fold_in(splits[7], 71), 0),
        "far": draw_far(jax.random.fold_in(splits[7], 71), 0),
        "skel": draw_skel(jax.random.fold_in(splits[7], 71), 0),
    }


def apply_tile(target, source, source_chg):
    cross = jnp.dot(target, source.T, precision=lax.Precision.HIGHEST, preferred_element_type=jnp.float32)
    dist_sq = jnp.sum(target * target, axis=1)[:, None] + jnp.sum(source * source, axis=1)[None, :] - 2.0 * cross
    kernel = jnp.exp(-dist_sq * (4.0 / target.shape[1]))
    return jnp.dot(kernel, source_chg, precision=lax.Precision.HIGHEST, preferred_element_type=jnp.float32)


def listed_sum(target, sources, source_chg):
    return jnp.sum(jax.vmap(lambda source, charge: apply_tile(target, source, charge))(sources, source_chg), axis=0)


def reference(points, charges, interp, order, near, far, skel):
    tree_ordered_points = jnp.zeros_like(points).at[order].set(points)
    tree_chg = jnp.zeros_like(charges).at[order].set(charges)
    leaf_total = near.shape[0]
    leaf_size = tree_ordered_points.shape[0] // leaf_total
    leaf_pts = tree_ordered_points.reshape(leaf_total, leaf_size, -1)
    leaf_charge_block = tree_chg.reshape(leaf_total, leaf_size, -1)
    leaf_interpolant = interp.reshape(leaf_total, leaf_size, -1)
    skel_pts = jnp.take_along_axis(leaf_pts, skel[:, :, None], axis=1)
    skeleton_charge = jnp.einsum("euq,eub->eqb", leaf_interpolant, leaf_charge_block, precision=lax.Precision.HIGHEST)

    def one_leaf(index):
        near_part = listed_sum(leaf_pts[index], leaf_pts[near[index]], leaf_charge_block[near[index]])
        skeleton_potential = listed_sum(skel_pts[index], skel_pts[far[index]], skeleton_charge[far[index]])
        far_field_part = jnp.dot(leaf_interpolant[index], skeleton_potential, precision=lax.Precision.HIGHEST, preferred_element_type=jnp.float32)
        return near_part + far_field_part

    tree_pot = lax.map(one_leaf, jnp.arange(leaf_total, dtype=jnp.int32))
    return tree_pot.reshape(tree_ordered_points.shape[0], -1)[order]
```

```python
import functools
import math

import jax
import jax.numpy as jnp
from jax import lax
from jax.experimental import pallas as pl
from jax.experimental.pallas import tpu as pltpu
from jax.sharding import PartitionSpec as P

F32 = jnp.float32
BF16 = jnp.bfloat16
LANES = 128
JOINT = ("outer", "inner")
VMEM = pl.BlockSpec(memory_space=pltpu.VMEM)
SMEM = pl.BlockSpec(memory_space=pltpu.SMEM)


def call(body, outs, args, in_specs, scratch=(), alias=None, flops=0, name=None, vmem=48):
    nbytes = sum(a.size * 4 for a in args) + sum(o.size * 4 for o in outs)
    return pl.pallas_call(
        body,
        out_shape=outs,
        in_specs=in_specs,
        out_specs=[VMEM] * len(outs),
        scratch_shapes=list(scratch),
        input_output_aliases=alias or {},
        compiler_params=pltpu.CompilerParams(vmem_limit_bytes=vmem << 20),
        cost_estimate=pl.CostEstimate(flops=flops, bytes_accessed=nbytes, transcendentals=0),
        name=name,
    )(*args)


def split(x):
    hi = x.astype(BF16)
    return hi, (x - hi.astype(F32)).astype(BF16)


def split3(x):
    a = x.astype(BF16)
    r = x - a.astype(F32)
    b = r.astype(BF16)
    return a, b, (r - b.astype(F32)).astype(BF16)


def unpack(packed, dim):
    return jnp.concatenate([packed[:, :dim], packed[:, dim : 2 * dim]], axis=0)


def pack(rows, dim):
    half = rows.shape[0] // 2
    return jnp.concatenate([rows[:half, :dim], rows[half:, :dim]], axis=1)


def norm_lanes(x, scale, first):
    n = -scale * jnp.sum(x * x, axis=1, keepdims=True)
    a, b, c = (v.astype(F32) for v in split3(n))
    lane = lax.broadcasted_iota(jnp.int32, x.shape, 1)
    base = 0 if first else 3
    ones = 3 if first else 0
    out = jnp.where((lane >= ones) & (lane < ones + 3), 1.0, 0.0)
    for j, v in enumerate((a, b, c)):
        out = jnp.where(lane == base + j, v, out)
    return out.astype(BF16)


def target_side(x, scale):
    hi, lo = split(x * (2.0 * scale))
    return jnp.concatenate([hi, lo, hi, norm_lanes(x, scale, True)], axis=1)


def source_side(x, scale):
    hi, lo = split(x)
    return jnp.concatenate([hi, hi, lo, norm_lanes(x, scale, False)], axis=1)


def charge_side(c):
    hi, lo = split(c)
    return jnp.concatenate([hi, lo], axis=1)


def nt_dot(a, b):
    return lax.dot_general(a, b, (((1,), (1,)), ((), ())), preferred_element_type=F32)


def tn_dot(a, b):
    return lax.dot_general(a, b, (((0,), (0,)), ((), ())), preferred_element_type=F32)


def fold(p):
    half = p.shape[1] // 2
    return p[:, :half] + p[:, half:]


def tile_product(target, source, charge):
    k = jnp.exp2(nt_dot(target, source))
    hi, lo = split(k)
    return fold(
        jnp.dot(hi, charge, preferred_element_type=F32)
        + jnp.dot(lo, charge, preferred_element_type=F32)
    )


def div_mod(x, n):
    if n & (n - 1) == 0:
        return lax.shift_right_logical(x, jnp.int32(n.bit_length() - 1)), x & (n - 1)
    q = lax.div(x, jnp.int32(n))
    return q, x - q * n


UNROLL = 16


def rows_loop(count, body):
    def step(i, carry):
        for u in range(UNROLL):
            body(i * UNROLL + u)
        return carry

    lax.fori_loop(0, count // UNROLL, step, 0)


def send_kernel(devs, pair, block, order_ref, pts_ref, chg_ref, send_ref, code_ref, ptmp, idx_v, idx_s, sem):
    rows = chg_ref.shape[0]
    dim = pts_ref.shape[1]
    lines = rows // LANES
    dest, slot = div_mod(order_ref[...], rows)
    sub = lax.broadcasted_iota(jnp.int32, (devs, LANES), 0)
    hot = [jnp.where(dest[r : r + 1, :] == sub, 1.0, 0.0) for r in range(lines)]
    ki = lax.broadcasted_iota(jnp.int32, (LANES, 2 * LANES), 0)
    ji = lax.broadcasted_iota(jnp.int32, (LANES, 2 * LANES), 1)
    tri = jnp.where((ki < ji) | (ji >= LANES), 1.0, 0.0).astype(BF16)
    pre = jnp.dot(jnp.concatenate([h.astype(BF16) for h in hot], axis=0), tri, preferred_element_type=F32)
    base = jnp.zeros((devs, LANES), F32)
    ranks = []
    for r in range(lines):
        part = pre[r * devs : (r + 1) * devs]
        ranks.append(jnp.sum(hot[r] * (part[:, :LANES] + base), axis=0, keepdims=True))
        base = base + part[:, LANES:]
    rank_f = jnp.concatenate(ranks, axis=0)
    rank = rank_f.astype(jnp.int32)
    idx_v[...] = dest * block + rank
    copy = pltpu.make_async_copy(idx_v, idx_s, sem)
    copy.start()
    code_ref[...] = dest * (2 * pair) + rank
    psub = lax.broadcasted_iota(jnp.int32, (pair, LANES), 0)
    s_hi = lax.shift_right_logical(slot, 8).astype(F32)
    s_lo = (slot & 255).astype(F32)
    left, right = [], []
    for r in range(lines):
        left.append(
            jnp.concatenate([hot[r] * s_hi[r : r + 1, :], hot[r] * s_lo[r : r + 1, :]], axis=0).astype(BF16)
        )
        right.append(jnp.where(rank[r : r + 1, :] == psub, 1.0, 0.0).astype(BF16))
    both = nt_dot(jnp.concatenate(left, axis=1), jnp.concatenate(right, axis=1))
    table = both[:devs] * 256.0 + both[devs:]
    if pair < LANES:
        table = jnp.concatenate([table, jnp.zeros((devs, LANES - pair), F32)], axis=1)
    copy.wait()

    def move(n):
        j = idx_s[n // LANES, n % LANES]
        send_ref[pl.ds(j, 1), :] = chg_ref[pl.ds(n, 1), :]
        ptmp[pl.ds(j, 1), :dim] = pts_ref[pl.ds(n, 1), :]

    rows_loop(rows, move)
    half = pair // 2
    for d in range(devs):
        send_ref[d * block + pair : d * block + pair + half, :] = pack(
            ptmp[d * block : d * block + pair, :], dim
        )
        send_ref[d * block + pair + half : (d + 1) * block, :] = jnp.broadcast_to(
            table[d : d + 1, :], (block - pair - half, LANES)
        )


def place_kernel(devs, pair, block, leaf, dim, recv_ref, ring_ref, pts_ref, exch_ref, pos_ref, rolled, pos_s, sem):
    half = pair // 2
    rows = pts_ref.shape[0]
    leaves = rows // leaf
    line = leaf + leaf // 2
    table = jnp.concatenate(
        [recv_ref[d * block + pair + half : d * block + pair + half + 1, :] for d in range(devs)], axis=0
    )
    pos_ref[...] = table.astype(jnp.int32)
    copy = pltpu.make_async_copy(pos_ref, pos_s, sem)
    copy.start()
    exch_ref[rows // 2 :, :] = table
    for d in range(devs):
        part = recv_ref[d * block + pair : d * block + pair + half, :]
        rolled[d * half : (d + 1) * half, :] = jnp.concatenate([part[:, dim:], part[:, :dim]], axis=1)
    copy.wait()

    def per_source(d, carry):
        for j in range(pair):
            p = pos_s[d, j]
            g, _ = div_mod(p, leaf)
            ring_ref[pl.ds(p + g * (line - leaf), 1), :] = recv_ref[pl.ds(d * block + j, 1), :]
            if j < half:
                pts_ref[pl.ds(p, 1), :] = recv_ref[pl.ds(d * block + pair + j, 1), :]
            else:
                pts_ref[pl.ds(p, 1), :] = rolled[pl.ds(d * half + j - half, 1), :]
        return carry

    lax.fori_loop(0, devs, per_source, 0)
    for g in range(leaves):
        packed = pack(pts_ref[g * leaf : (g + 1) * leaf, :], dim)
        ring_ref[g * line + leaf : (g + 1) * line, :] = packed
        exch_ref[g * (leaf // 2) : (g + 1) * (leaf // 2), :] = packed


def skeleton_kernel(leaf, dim, ring_ref, pts_ref, interp_ref, skel_ref, far_ref, stmp):
    leaves, skel = skel_ref.shape
    line = leaf + leaf // 2
    fline = skel + skel // 2

    for g in range(leaves):

        def move(n, g=g):
            stmp[pl.ds(g * skel + n, 1), :] = pts_ref[pl.ds(g * leaf + skel_ref[g, n], 1), :]

        rows_loop(skel, move)
    for g in range(leaves):
        hi, lo = split(interp_ref[g * leaf : (g + 1) * leaf, :])
        charge = charge_side(ring_ref[g * line : g * line + leaf, :])
        far_ref[g * fline : g * fline + skel, :] = fold(tn_dot(hi, charge) + tn_dot(lo, charge))
        far_ref[g * fline + skel : (g + 1) * fline, :] = pack(stmp[g * skel : (g + 1) * skel, :], dim)


def far_kernel(skel, dim, scale, n_inner, blocks, far_rows_ref, own_ref, interp_ref, *rest):
    refs, (out_ref, src, chg) = rest[:blocks], rest[blocks:]
    leaves, fars = far_rows_ref.shape
    leaf = interp_ref.shape[0] // leaves
    fline = skel + skel // 2
    outer = lax.axis_index("outer")
    for b in range(blocks):
        for g in range(leaves):
            at = b * leaves + g
            src[at] = source_side(unpack(refs[b][g * fline + skel : (g + 1) * fline, :], dim), scale)
            chg[at] = charge_side(refs[b][g * fline : g * fline + skel, :])

    for g in range(leaves):
        target = target_side(unpack(own_ref[g * fline + skel : (g + 1) * fline, :], dim), scale)
        q = jnp.zeros((skel, LANES), F32)
        for k in range(fars):
            device, local = div_mod(far_rows_ref[g, k], leaves)
            at = ((device // n_inner) ^ outer) * leaves - leaves + local
            q = q + tile_product(target, src[at], chg[at])
        qq = charge_side(q)
        hi, lo = split(interp_ref[g * leaf : (g + 1) * leaf, :])
        out_ref[g * leaf : (g + 1) * leaf, :] = fold(
            jnp.dot(hi, qq, preferred_element_type=F32) + jnp.dot(lo, qq, preferred_element_type=F32)
        )


def target_kernel(leaf, dim, scale, packed_ref, out_ref):
    for g in range(out_ref.shape[0]):
        x = unpack(packed_ref[g * (leaf // 2) : (g + 1) * (leaf // 2), :], dim)
        out_ref[g] = target_side(x, scale)


def near_kernel(leaf, dim, scale, leaves, parts, fresh, *refs):
    near_ref, who_ref, own_ref, partner_ref = refs[:4]
    sources = refs[4 : 4 + len(parts)]
    rest = refs[4 + len(parts) :]
    acc_ref, src, chg = rest[-3:]
    line = leaf + leaf // 2
    n_near = near_ref.shape[1]
    at = 0
    for ref, (first, count) in zip(sources, parts):
        for g in range(count):
            src[at + g] = source_side(unpack(ref[g * line + leaf : (g + 1) * line, :], dim), scale)
            chg[at + g] = charge_side(ref[g * line : g * line + leaf, :])
        at += count
    acc_ref[...] = jnp.zeros_like(acc_ref) if fresh else rest[0][...]

    step = leaf // 2

    def one(side, target_ref, t, k):
        device, local = div_mod(near_ref[side * leaves + t, k], leaves)
        at = 0
        for b, (first, count) in enumerate(parts):
            hit = (device == who_ref[b]) & (local >= first) & (local < first + count)
            index = at - first + local
            at += count

            @pl.when(hit)
            def _():
                for c in range(0, leaf, step):
                    rows = pl.ds(pl.multiple_of((side * leaves + t) * leaf + c, step), step)
                    acc_ref[rows, :] += tile_product(
                        target_ref[t, c : c + step, :], src[index], chg[index]
                    )

    for side, target_ref in enumerate((own_ref, partner_ref)):

        def entry(e, carry, side=side, target_ref=target_ref):
            t, k = div_mod(e, n_near)
            one(side, target_ref, t, k)
            return carry

        lax.fori_loop(0, leaves * n_near, entry, 0)


def return_kernel(devs, pair, acc_ref, far_ref, pos_ref, other_ref, out_ref, total, opos_v, opos_s, sem):
    rows = far_ref.shape[0]
    opos_v[...] = other_ref[...].astype(jnp.int32)
    copy = pltpu.make_async_copy(opos_v, opos_s, sem)
    copy.start()
    total[...] = acc_ref[:rows, :] + far_ref[...]
    copy.wait()

    def per_source(d, carry):
        for j in range(pair):
            out_ref[pl.ds(d * 2 * pair + j, 1), :] = total[pl.ds(pos_ref[d, j], 1), :]
            out_ref[pl.ds(d * 2 * pair + pair + j, 1), :] = acc_ref[pl.ds(rows + opos_s[d, j], 1), :]
        return carry

    lax.fori_loop(0, devs, per_source, 0)


def final_kernel(pair, n_inner, ret_ref, code_ref, out_ref):
    flip = (n_inner // 2) * 2 * pair

    def move(n):
        c = code_ref[n // LANES, n % LANES]
        out_ref[pl.ds(n, 1), :] = ret_ref[pl.ds(c, 1), :] + ret_ref[pl.ds((c ^ flip) + pair, 1), :]

    rows_loop(out_ref.shape[0], move)


def shards(points, charges, interp, order, near, far, skel):
    n_inner = lax.axis_size("inner")
    n_outer = lax.axis_size("outer")
    devs = n_inner * n_outer
    rows, dim = points.shape
    leaves, n_skel = skel.shape
    leaf = rows // leaves
    line = leaf + leaf // 2
    fline = n_skel + n_skel // 2
    pair = rows // devs
    block = pair + pair // 2 + 8
    scale = (4.0 / dim) * math.log2(math.e)
    outer = lax.axis_index("outer")
    inner = lax.axis_index("inner")
    me = outer * n_inner + inner
    half = n_inner // 2
    partner = outer * n_inner + (inner ^ half)

    def f32(*shape):
        return jax.ShapeDtypeStruct(shape, F32)

    def i32(*shape):
        return jax.ShapeDtypeStruct(shape, jnp.int32)

    def near_of(device):
        return lax.dynamic_slice_in_dim(near, device * leaves, leaves, 0)

    near_rows = jnp.concatenate([near_of(me), near_of(partner)], axis=0)
    far_rows = lax.dynamic_slice_in_dim(far, me * leaves, leaves, 0)

    send, code = call(
        functools.partial(send_kernel, devs, pair, block),
        [f32(devs * block, LANES), i32(rows // LANES, LANES)],
        (order.reshape(rows // LANES, LANES), points, charges),
        [VMEM] * 3,
        [
            pltpu.VMEM((devs * block, LANES), F32),
            pltpu.VMEM((rows // LANES, LANES), jnp.int32),
            pltpu.SMEM((rows // LANES, LANES), jnp.int32),
            pltpu.SemaphoreType.DMA,
        ],
        name="send",
    )
    recv = lax.all_to_all(send.reshape(devs, block, LANES), JOINT, 0, 0, tiled=True)
    ring, pts, exch, pos = call(
        functools.partial(place_kernel, devs, pair, block, leaf, dim),
        [f32(leaves * line, LANES), f32(rows, LANES), f32(rows // 2 + devs, LANES), i32(devs, LANES)],
        (recv.reshape(devs * block, LANES),),
        [VMEM],
        [
            pltpu.VMEM((devs * pair // 2, LANES), F32),
            pltpu.SMEM((devs, LANES), jnp.int32),
            pltpu.SemaphoreType.DMA,
        ],
        name="place",
    )

    loop = [j ^ (j >> 1) for j in range(half)]
    right = [
        (base + loop[j], base + loop[(j + 1) % half]) for base in (0, half) for j in range(half)
    ]
    left = [(b, a) for a, b in right]
    place_of = jnp.asarray([loop.index(j % half) for j in range(n_inner)], jnp.int32)
    member = jnp.asarray(loop, jnp.int32)

    def owner(offset):
        at = place_of[inner] + offset
        return outer * n_inner + (inner // half) * half + member[at % half]

    from_left, from_right = ring, ring
    arrivals = []
    for step in range(1, half // 2):
        from_left = lax.ppermute(from_left, "inner", right)
        from_right = lax.ppermute(from_right, "inner", left)
        arrivals.append((((from_left, 0, leaves, -step),), ((from_right, 0, leaves, step),)))
    theirs = lax.ppermute(exch, "inner", [(i, i ^ half) for i in range(n_inner)])
    cut = leaves // 2
    low = lax.ppermute(from_left[: cut * line], "inner", right)
    high = lax.ppermute(from_right[cut * line :], "inner", left)

    (far_own,) = call(
        functools.partial(skeleton_kernel, leaf, dim),
        [f32(leaves * fline, LANES)],
        (ring, pts, interp, skel),
        [VMEM, VMEM, VMEM, SMEM],
        [pltpu.VMEM((leaves * n_skel, LANES), F32)],
        flops=2 * rows * n_skel * 3 * 128,
        name="skeleton",
    )
    held = {0: far_own}
    bit = n_outer // 2
    while bit:
        perm = [(o, o ^ bit) for o in range(n_outer)]
        held.update({r ^ bit: lax.ppermute(v, "outer", perm) for r, v in list(held.items())})
        bit //= 2

    targets = []
    for packed in (exch, theirs):
        (t,) = call(
            functools.partial(target_kernel, leaf, dim, scale),
            [jax.ShapeDtypeStruct((leaves, leaf, 4 * dim), BF16)],
            (packed,),
            [VMEM],
            name="targets",
        )
        targets.append(t)

    def near_call(acc, pieces):
        parts = tuple((first, count) for _, first, count, _ in pieces)
        who = jnp.stack([owner(offset) for _, _, _, offset in pieces])
        total = sum(count for _, count in parts)
        args = (near_rows, who, *targets, *(p[0] for p in pieces))
        specs = [SMEM, SMEM] + [VMEM] * (2 + len(pieces))
        alias = {}
        if acc is not None:
            alias = {len(args): 0}
            args += (acc,)
            specs.append(VMEM)
        return call(
            functools.partial(near_kernel, leaf, dim, scale, leaves, parts, acc is None),
            [f32(2 * rows, LANES)],
            args,
            specs,
            [
                pltpu.VMEM((total, leaf, 4 * dim), BF16),
                pltpu.VMEM((total, leaf, 2 * LANES), BF16),
            ],
            alias,
            flops=total * 2 * leaf * leaf * 256 * 3 * 2,
            name="near",
        )[0]

    acc = near_call(None, ((ring, 0, leaves, 0),))
    for a, b in arrivals:
        acc = near_call(acc, a)
        acc = near_call(acc, b)
    others = [held[r] for r in range(1, n_outer)]
    n_blocks = len(others) * leaves
    (far_part,) = call(
        functools.partial(far_kernel, n_skel, dim, scale, n_inner, len(others)),
        [f32(rows, LANES)],
        (far_rows, far_own, interp, *others),
        [SMEM] + [VMEM] * (2 + len(others)),
        [
            pltpu.VMEM((n_blocks, n_skel, 4 * dim), BF16),
            pltpu.VMEM((n_blocks, n_skel, 2 * LANES), BF16),
        ],
        flops=leaves * 8 * 2 * n_skel * n_skel * 256 * 3,
        name="far",
    )
    opposite = half // 2
    acc = near_call(acc, ((low, 0, cut, opposite), (high, cut, leaves - cut, opposite)))

    (out,) = call(
        functools.partial(return_kernel, devs, pair),
        [f32(devs * 2 * pair, LANES)],
        (acc, far_part, pos, theirs[rows // 2 :]),
        [VMEM, VMEM, SMEM, VMEM],
        [
            pltpu.VMEM((rows, LANES), F32),
            pltpu.VMEM((devs, LANES), jnp.int32),
            pltpu.SMEM((devs, LANES), jnp.int32),
            pltpu.SemaphoreType.DMA,
        ],
        name="outgoing",
    )
    returned = lax.all_to_all(out.reshape(devs, 2 * pair, LANES), JOINT, 0, 0, tiled=True)
    (final,) = call(
        functools.partial(final_kernel, pair, n_inner),
        [f32(rows, LANES)],
        (returned.reshape(devs * 2 * pair, LANES), code),
        [VMEM, SMEM],
        name="final",
    )
    return final


def solution(mesh):
    row = P(JOINT, None)
    in_specs = (row, row, row, P(JOINT), P(), P(), row)
    return jax.shard_map(shards, mesh=mesh, in_specs=in_specs, out_specs=row, check_vma=False)
```

```python
import functools
import math

import jax
import jax.numpy as jnp
from jax import lax
from jax.experimental import pallas as pl
from jax.experimental.pallas import tpu as pltpu
from jax.sharding import PartitionSpec as P


F32 = jnp.float32
BF16 = jnp.bfloat16
LANES = 128
JOINT = ("outer", "inner")
VMEM = pl.BlockSpec(memory_space=pltpu.VMEM)
SMEM = pl.BlockSpec(memory_space=pltpu.SMEM)
HBM = pl.BlockSpec(memory_space=pltpu.HBM)


def call(body, outs, args, in_specs, scratch=(), out_specs=None, flops=0):
    nbytes = sum(a.size * a.dtype.itemsize for a in (*args, *outs))
    held = sum(math.prod(s.shape) * jnp.dtype(s.dtype).itemsize for s in scratch if getattr(s, "memory_space", None) == pltpu.VMEM)
    limit = min(60 << 20, nbytes + held + (8 << 20))
    return pl.pallas_call(
        body,
        out_shape=outs,
        in_specs=in_specs,
        out_specs=out_specs or [VMEM] * len(outs),
        scratch_shapes=list(scratch),
        compiler_params=pltpu.CompilerParams(vmem_limit_bytes=limit),
        cost_estimate=pl.CostEstimate(flops=flops, bytes_accessed=nbytes, transcendentals=0),
    )(*args)


def split(x):
    hi = x.astype(BF16)
    return hi, (x - hi.astype(F32)).astype(BF16)


def pack(rows, dim):
    half = rows.shape[0] // 2
    return jnp.concatenate([rows[:half, :dim], rows[half:, :dim]], axis=1)


def exponent_side(packed, dim, scale, is_target):
    lane = lax.broadcasted_iota(jnp.int32, packed.shape, 1)
    first = lane < dim
    turned = jnp.concatenate([packed[:, dim:], packed[:, :dim]], axis=1)
    at = dim + (0 if is_target else 3)
    ones = jnp.where((lane >= dim) & (lane < dim + 6), 1.0, 0.0)
    blocks = []
    for x in (jnp.where(first, packed, turned), jnp.where(first, turned, packed)):
        n = jnp.sum(x * x, axis=1, keepdims=True) * (-0.5 * scale)
        norms = jnp.where(lane == at, n, ones)
        for j in (1, 2):
            n = n - n.astype(BF16).astype(F32)
            norms = jnp.where(lane == at + j, n, norms)
        if is_target:
            x = x * (2.0 * scale)
        low = x - x.astype(BF16).astype(F32)
        if is_target:
            head, tail = jnp.where(first, x, low), jnp.where(first, x, norms)
        else:
            head, tail = x, jnp.where(first, low, norms)
        blocks.append(jnp.concatenate([head, tail], axis=1).astype(BF16))
    return blocks


def load_points(ref, pitch, skip, base, out, scale, is_target):
    count = ref.shape[0] // pitch
    size = out.shape[1] // 2
    step = size
    parts = size // step

    def body(i, carry):
        g, c = div_mod(i, parts)
        at = pl.multiple_of(g * pitch + skip + c * step, 8)
        blocks = exponent_side(ref[pl.ds(at, step), :], LANES // 2, scale, is_target)
        for j, value in enumerate(blocks):
            out[base + g, pl.ds(pl.multiple_of(j * size + c * step, step), step), :] = value
        return carry

    lax.fori_loop(0, count * parts, body, 0)


def load_charges(ref, pitch, base, out):
    count = ref.shape[0] // pitch
    step = 256
    parts = out.shape[1] // step

    def body(i, carry):
        g, c = div_mod(i, parts)
        at = pl.multiple_of(g * pitch + c * step, 8)
        hi, lo = split(ref[pl.ds(at, step), :])
        rows = pl.ds(pl.multiple_of(c * step, step), step)
        out[base + g, rows, :LANES] = hi
        out[base + g, rows, LANES:] = lo
        return carry

    lax.fori_loop(0, count * parts, body, 0)


def charge_side(c):
    hi, lo = split(c)
    return jnp.concatenate([hi, lo], axis=1)


def nt_dot(a, b):
    return lax.dot_general(a, b, (((1,), (1,)), ((), ())), preferred_element_type=F32)


def tn_dot(a, b):
    return lax.dot_general(a, b, (((0,), (0,)), ((), ())), preferred_element_type=F32)


def fold(p):
    half = p.shape[1] // 2
    return p[:, :half] + p[:, half:]


def tile_product(target, source, charge):
    k = jnp.exp2(nt_dot(target, source))
    hi, lo = split(k)
    return fold(
        jnp.dot(hi, charge, preferred_element_type=F32)
        + jnp.dot(lo, charge, preferred_element_type=F32)
    )


def div_mod(x, n):
    if n & (n - 1) == 0:
        return lax.shift_right_logical(x, jnp.int32(n.bit_length() - 1)), x & (n - 1)
    q = lax.div(x, jnp.int32(n))
    return q, x - q * n


UNROLL = 64


def rows_loop(count, body):
    def step(i, carry):
        line, part = div_mod(i, LANES // UNROLL)
        for u in range(UNROLL):
            body(i * UNROLL + u, line, part * UNROLL + u)
        return carry

    lax.fori_loop(0, count // UNROLL, step, 0)


def send_kernel(devs, pair, block, order_hbm, pts_hbm, chg_hbm, send_ref, code_ref, ptmp, prow, order_ref, pts_ref, chg_ref, idx_v, idx_s, sem, sems):
    loads = [
        pltpu.make_async_copy(a, b, sems.at[i])
        for i, (a, b) in enumerate(((order_hbm, order_ref), (chg_hbm, chg_ref), (pts_hbm, pts_ref)))
    ]
    for load in loads:
        load.start()
    loads[0].wait()
    rows = chg_ref.shape[0]
    dim = pts_ref.shape[0]
    lines = rows // LANES
    dest, slot = div_mod(order_ref[...], rows)
    sub = lax.broadcasted_iota(jnp.int32, (devs, LANES), 0)
    hot = [jnp.where(dest[r : r + 1, :] == sub, 1.0, 0.0) for r in range(lines)]
    ki = lax.broadcasted_iota(jnp.int32, (LANES, 2 * LANES), 0)
    ji = lax.broadcasted_iota(jnp.int32, (LANES, 2 * LANES), 1)
    tri = jnp.where((ki < ji) | (ji >= LANES), 1.0, 0.0).astype(BF16)
    pre = jnp.dot(jnp.concatenate([h.astype(BF16) for h in hot], axis=0), tri, preferred_element_type=F32)
    base = jnp.zeros((devs, LANES), F32)
    ranks = []
    for r in range(lines):
        part = pre[r * devs : (r + 1) * devs]
        ranks.append(jnp.sum(hot[r] * (part[:, :LANES] + base), axis=0, keepdims=True))
        base = base + part[:, LANES:]
    rank_f = jnp.concatenate(ranks, axis=0)
    rank = rank_f.astype(jnp.int32)
    idx_v[...] = dest * block + rank
    copy = pltpu.make_async_copy(idx_v, idx_s, sem)
    copy.start()
    code_ref[...] = dest * pair + rank
    psub = lax.broadcasted_iota(jnp.int32, (pair, LANES), 0)
    s_hi = lax.shift_right_logical(slot, 8).astype(F32)
    s_lo = (slot & 255).astype(F32)
    left, right = [], []
    for r in range(lines):
        left.append(
            jnp.concatenate([hot[r] * s_hi[r : r + 1, :], hot[r] * s_lo[r : r + 1, :]], axis=0).astype(BF16)
        )
        right.append(jnp.where(rank[r : r + 1, :] == psub, 1.0, 0.0).astype(BF16))
    both = nt_dot(jnp.concatenate(left, axis=1), jnp.concatenate(right, axis=1))
    table = both[:devs] * 256.0 + both[devs:]
    if pair < LANES:
        table = jnp.concatenate([table, jnp.zeros((devs, LANES - pair), F32)], axis=1)
    loads[2].wait()
    for c in range(0, rows, 256):
        prow[c : c + 256, :dim] = pts_ref[:, c : c + 256].T
    loads[1].wait()
    copy.wait()

    def move(n, line, lane):
        j = idx_s[line, lane]
        send_ref[pl.ds(j, 1), :] = chg_ref[pl.ds(n, 1), :]
        ptmp[pl.ds(j, 1), :] = prow[pl.ds(n, 1), :]

    rows_loop(rows, move)
    half = pair // 2
    for d in range(devs):
        send_ref[d * block + pair : d * block + pair + half, :] = pack(
            ptmp[d * block : d * block + pair, :], dim
        )
        send_ref[d * block + pair + half : (d + 1) * block, :] = jnp.broadcast_to(
            table[d : d + 1, :], (block - pair - half, LANES)
        )


def place_kernel(devs, pair, block, leaf, dim, recv_ref, low_ref, high_ref, pts_ref, exch_ref, pos_ref, rolled, chg, pos_s, sem):
    half = pair // 2
    rows = pts_ref.shape[0]
    leaves = rows // leaf
    line = leaf + leaf // 2
    table = jnp.concatenate(
        [recv_ref[d * block + pair + half : d * block + pair + half + 1, :] for d in range(devs)], axis=0
    )
    pos_ref[...] = table.astype(jnp.int32)
    copy = pltpu.make_async_copy(pos_ref, pos_s, sem)
    copy.start()
    exch_ref[rows // 2 :, :] = table
    for d in range(devs):
        part = recv_ref[d * block + pair : d * block + pair + half, :]
        rolled[d * half : (d + 1) * half, :] = jnp.concatenate([part[:, dim:], part[:, :dim]], axis=1)
    copy.wait()

    def per_source(d, carry):
        for j in range(pair):
            p = pos_s[d, j]
            chg[pl.ds(p, 1), :] = recv_ref[pl.ds(d * block + j, 1), :]
            if j < half:
                pts_ref[pl.ds(p, 1), :] = recv_ref[pl.ds(d * block + pair + j, 1), :]
            else:
                pts_ref[pl.ds(p, 1), :] = rolled[pl.ds(d * half + j - half, 1), :]
        return carry

    lax.fori_loop(0, devs, per_source, 0)
    for g in range(leaves):
        packed = pack(pts_ref[g * leaf : (g + 1) * leaf, :], dim)
        ref, at = (low_ref, g * line) if g < leaves // 2 else (high_ref, (g - leaves // 2) * line)
        ref[at : at + leaf, :] = chg[g * leaf : (g + 1) * leaf, :]
        ref[at + leaf : at + line, :] = packed
        exch_ref[g * (leaf // 2) : (g + 1) * (leaf // 2), :] = packed


def skeleton_kernel(leaf, dim, low_ref, high_ref, pts_ref, interp_ref, skel_ref, far_ref, stmp):
    leaves, skel = skel_ref.shape
    line = leaf + leaf // 2
    fline = skel + skel // 2

    for g in range(leaves):

        def move(n, line, lane, g=g):
            stmp[pl.ds(g * skel + n, 1), :] = pts_ref[pl.ds(g * leaf + skel_ref[g, n], 1), :]

        rows_loop(skel, move)
    for g in range(leaves):
        hi, lo = split(interp_ref[g * leaf : (g + 1) * leaf, :])
        ref, at = (low_ref, g * line) if g < leaves // 2 else (high_ref, (g - leaves // 2) * line)
        charge = charge_side(ref[at : at + leaf, :])
        far_ref[g * fline : g * fline + skel, :] = fold(tn_dot(hi, charge) + tn_dot(lo, charge))
        far_ref[g * fline + skel : (g + 1) * fline, :] = pack(stmp[g * skel : (g + 1) * skel, :], dim)


def far_kernel(skel, scale, n_inner, blocks, far_rows_ref, own_ref, interp_ref, *rest):
    refs, (out_ref, src, chg, tgt) = rest[:blocks], rest[blocks:]
    leaves, fars = far_rows_ref.shape
    leaf = interp_ref.shape[0] // leaves
    fline = skel + skel // 2
    outer = lax.axis_index("outer")
    for b in range(blocks):
        load_points(refs[b], fline, skel, b * leaves, src, scale, False)
        load_charges(refs[b], fline, b * leaves, chg)
    load_points(own_ref, fline, skel, 0, tgt, scale, True)

    for g in range(leaves):
        q = jnp.zeros((skel, LANES), F32)
        for k in range(fars):
            device, local = div_mod(far_rows_ref[g, k], leaves)
            at = ((device // n_inner) ^ outer) * leaves - leaves + local
            q = q + tile_product(tgt[g], src[at], chg[at])
        qq = charge_side(q)
        hi, lo = split(interp_ref[g * leaf : (g + 1) * leaf, :])
        out_ref[g * leaf : (g + 1) * leaf, :] = fold(
            jnp.dot(hi, qq, preferred_element_type=F32) + jnp.dot(lo, qq, preferred_element_type=F32)
        )


def ring_place(member, bits):
    place, shift = member, 1
    while shift < bits:
        place = place ^ lax.shift_right_logical(member, jnp.int32(shift))
        shift += 1
    return place


def target_kernel(leaf, scale, own_ref, theirs_ref, out_ref):
    leaves = out_ref.shape[0] // 2
    for j, ref in enumerate((own_ref, theirs_ref)):
        load_points(ref.at[: leaves * leaf // 2], leaf // 2, 0, j * leaves, out_ref, scale, True)


CODE = 1024
GROUP = 2


def list_kernel(leaves, n_inner, near_ref, list_ref, count_ref):
    half = n_inner // 2
    n_near = near_ref.shape[1]
    bits = half.bit_length() - 1
    inner = lax.axis_index("inner")
    mine = ring_place(inner & (half - 1), bits)
    count_ref[0] = 0
    count_ref[1] = 0

    def add(row, code):
        n = count_ref[row]
        list_ref[row, n] = code
        count_ref[row] = n + 1

    def entry(e, carry):
        row, k = div_mod(e, n_near)
        device, local = div_mod(near_ref[row, k], leaves)
        member = device & (n_inner - 1)
        same_half = (member ^ inner) < half
        offset = (ring_place(member & (half - 1), bits) - mine) & (half - 1)
        slot = jnp.where(offset > half // 2, 2 * (half - offset) - 1, 2 * offset)

        @pl.when(same_half & (offset == half // 2))
        def _():
            add(1, row * CODE + local)

        @pl.when(same_half & (offset != half // 2) & ((member != inner) | (row >= leaves)))
        def _():
            add(0, row * CODE + slot * leaves + local)

        return carry

    lax.fori_loop(0, 2 * leaves * n_near, entry, 0)
    for row in range(2):
        for _ in range(GROUP - 1):

            @pl.when(count_ref[row] % GROUP != 0)
            def _():
                add(row, 2 * leaves * CODE)


def load_sources(leaf, scale, refs, src, chg):
    line = leaf + leaf // 2
    at = 0
    for ref in refs:
        load_points(ref, line, leaf, at, src, scale, False)
        load_charges(ref, line, at, chg)
        at += ref.shape[0] // line


def leaf_rows(t, c, leaf, step):
    return pl.ds(pl.multiple_of(t * leaf + c, step), step)


def self_kernel(leaf, scale, own_ref, low_ref, high_ref, acc_ref, src, chg, tgt):
    leaves = src.shape[0]
    load_sources(leaf, scale, (low_ref, high_ref), src, chg)
    load_points(own_ref.at[: leaves * leaf // 2], leaf // 2, 0, 0, tgt, scale, True)
    step = leaf // 2

    def entry(t, carry):
        for c in range(0, leaf, step):
            acc_ref[leaf_rows(t, c, leaf, step), :] = tile_product(
                tgt[t, c : c + step, :], src[t], chg[t]
            )
        return carry

    lax.fori_loop(0, leaves, entry, 0)


def add_listed(leaf, row, list_ref, count_ref, tgt, src, chg, acc):
    step = leaf // 2

    def entry(e, carry):
        for u in range(GROUP):
            t, at = div_mod(list_ref[row, e * GROUP + u], CODE)
            x = jnp.minimum(t, tgt.shape[0] - 1)
            for c in range(0, leaf, step):
                acc[leaf_rows(t, c, leaf, step), :] += tile_product(
                    tgt[x, c : c + step, :], src[at], chg[at]
                )
        return carry

    lax.fori_loop(0, lax.shift_right_logical(count_ref[row], jnp.int32(GROUP.bit_length() - 1)), entry, 0)


def near_kernel(leaf, scale, list_ref, count_ref, tgt_ref, *rest):
    *sources, acc_ref, src, chg = rest
    load_sources(leaf, scale, sources, src, chg)
    acc_ref[...] = jnp.zeros_like(acc_ref)
    add_listed(leaf, 0, list_ref, count_ref, tgt_ref, src, chg, acc_ref)


def last_kernel(devs, pair, leaf, scale, list_ref, count_ref, pos_ref, tgt_ref, low_ref, high_ref, old_ref, self_ref, far_ref, other_ref, out_ref, acc, src, chg, opos_v, opos_s, sem):
    rows = far_ref.shape[0]
    opos_v[...] = other_ref[...].astype(jnp.int32)
    copy = pltpu.make_async_copy(opos_v, opos_s, sem)
    copy.start()
    load_sources(leaf, scale, (low_ref, high_ref), src, chg)
    acc[:rows, :] = old_ref[:rows, :] + (self_ref[...] + far_ref[...])
    acc[rows:, :] = old_ref[rows:, :]
    add_listed(leaf, 1, list_ref, count_ref, tgt_ref, src, chg, acc)
    copy.wait()

    def per_source(d, carry):
        for j in range(pair):
            out_ref[pl.ds(d * 2 * pair + j, 1), :] = acc[pl.ds(pos_ref[d, j], 1), :]
            out_ref[pl.ds(d * 2 * pair + pair + j, 1), :] = acc[pl.ds(rows + opos_s[d, j], 1), :]
        return carry

    lax.fori_loop(0, devs, per_source, 0)


def final_kernel(pair, n_inner, ret_ref, code_ref, out_ref, both):
    devs = both.shape[0] // pair
    for d in range(devs):
        other = d ^ (n_inner // 2)
        both[d * pair : (d + 1) * pair, :] = (
            ret_ref[2 * d * pair : (2 * d + 1) * pair, :]
            + ret_ref[(2 * other + 1) * pair : (2 * other + 2) * pair, :]
        )

    def move(n, line, lane):
        out_ref[pl.ds(n, 1), :] = both[pl.ds(code_ref[line, lane], 1), :]

    rows_loop(out_ref.shape[0], move)


def shards(points, charges, interp, order, near, far, skel):
    n_inner = lax.axis_size("inner")
    n_outer = lax.axis_size("outer")
    devs = n_inner * n_outer
    rows, dim = points.shape
    leaves, n_skel = skel.shape
    leaf = rows // leaves
    line = leaf + leaf // 2
    fline = n_skel + n_skel // 2
    pair = rows // devs
    block = pair + pair // 2 + 8
    scale = (4.0 / dim) * math.log2(math.e)
    outer = lax.axis_index("outer")
    inner = lax.axis_index("inner")
    me = outer * n_inner + inner
    half = n_inner // 2
    partner = outer * n_inner + (inner ^ half)

    def f32(*shape):
        return jax.ShapeDtypeStruct(shape, F32)

    def i32(*shape):
        return jax.ShapeDtypeStruct(shape, jnp.int32)

    def near_of(device):
        return lax.dynamic_slice_in_dim(near, device * leaves, leaves, 0)

    near_rows = jnp.concatenate([near_of(me), near_of(partner)], axis=0)
    far_rows = lax.dynamic_slice_in_dim(far, me * leaves, leaves, 0)

    send, code = call(
        functools.partial(send_kernel, devs, pair, block),
        [f32(devs * block, LANES), i32(rows // LANES, LANES)],
        (order.reshape(rows // LANES, LANES), points.T, charges),
        [HBM] * 3,
        [
            pltpu.VMEM((devs * block, LANES), F32),
            pltpu.VMEM((rows, LANES), F32),
            pltpu.VMEM((rows // LANES, LANES), jnp.int32),
            pltpu.VMEM((dim, rows), F32),
            pltpu.VMEM((rows, LANES), F32),
            pltpu.VMEM((rows // LANES, LANES), jnp.int32),
            pltpu.SMEM((rows // LANES, LANES), jnp.int32),
            pltpu.SemaphoreType.DMA,
            pltpu.SemaphoreType.DMA((3,)),
        ],
    )
    recv = lax.all_to_all(send.reshape(devs, block, LANES), JOINT, 0, 0, tiled=True)
    piece = leaves // 2 * line
    own_low, own_high, pts, exch, pos = call(
        functools.partial(place_kernel, devs, pair, block, leaf, dim),
        [f32(piece, LANES), f32(piece, LANES), f32(rows, LANES), f32(rows // 2 + devs, LANES), i32(devs, LANES)],
        (recv.reshape(devs * block, LANES),),
        [VMEM],
        [
            pltpu.VMEM((devs * pair // 2, LANES), F32),
            pltpu.VMEM((rows, LANES), F32),
            pltpu.SMEM((devs, LANES), jnp.int32),
            pltpu.SemaphoreType.DMA,
        ],
    )

    loop = [j ^ (j >> 1) for j in range(half)]
    right = [
        (base + loop[j], base + loop[(j + 1) % half]) for base in (0, half) for j in range(half)
    ]
    left = [(b, a) for a, b in right]

    def shift(x, perm):
        return lax.ppermute(x, "inner", perm)

    blocks = {0: (own_low, own_high)}
    to_right = to_left = (own_low, own_high)
    for step in range(1, half // 2):
        ra = shift(to_right[0], right)
        lb = shift(to_left[1], left)
        rb = shift(to_right[1], right)
        la = shift(to_left[0], left)
        to_right, to_left = (ra, rb), (la, lb)
        blocks[half - step], blocks[step] = to_right, to_left
    theirs = shift(exch, [(i, i ^ half) for i in range(n_inner)])
    blocks[half // 2] = (shift(to_right[0], right), shift(to_left[1], left))

    (far_own,) = call(
        functools.partial(skeleton_kernel, leaf, dim),
        [f32(leaves * fline, LANES)],
        (own_low, own_high, pts, interp, skel),
        [VMEM, VMEM, VMEM, VMEM, SMEM],
        [pltpu.VMEM((leaves * n_skel, LANES), F32)],
        flops=2 * rows * n_skel * 3 * 128,
    )
    held = {0: far_own}
    bit = n_outer // 2
    while bit:
        perm = [(o, o ^ bit) for o in range(n_outer)]
        got = {}
        for r, v in held.items():
            got[r ^ bit] = lax.ppermute(v, "outer", perm)
        held.update(got)
        bit //= 2

    lists, counts = call(
        functools.partial(list_kernel, leaves, n_inner),
        [i32(2, 2 * leaves * near.shape[1]), i32(2)],
        (near_rows,),
        [SMEM],
        out_specs=[SMEM, SMEM],
    )

    def tiles(count):
        return [
            pltpu.VMEM((count, leaf, 4 * dim), BF16),
            pltpu.VMEM((count, leaf, 2 * LANES), BF16),
        ]

    per_leaf = 2 * leaf * leaf * 256 * 3
    (own_sum,) = call(
        functools.partial(self_kernel, leaf, scale),
        [f32(rows, LANES)],
        (exch, own_low, own_high),
        [VMEM] * 3,
        tiles(leaves) + tiles(leaves)[:1],
        flops=leaves * per_leaf,
    )
    (targets,) = call(
        functools.partial(target_kernel, leaf, scale),
        [jax.ShapeDtypeStruct((2 * leaves, leaf, 4 * dim), BF16)],
        (exch, theirs),
        [VMEM] * 2,
        flops=1 << 20,
    )
    early = [0] + [j for step in range(1, half // 2) for j in (half - step, step)]
    sources = [piece for j in early for piece in blocks[j]]
    (acc,) = call(
        functools.partial(near_kernel, leaf, scale),
        [f32(2 * rows + leaf, LANES)],
        (lists, counts, targets, *sources),
        [SMEM, SMEM] + [VMEM] * (1 + len(sources)),
        tiles(len(early) * leaves),
        flops=len(early) * 2 * leaves * per_leaf,
    )
    others = [held[r] for r in range(1, n_outer)]
    n_blocks = len(others) * leaves
    (far_part,) = call(
        functools.partial(far_kernel, n_skel, scale, n_inner, len(others)),
        [f32(rows, LANES)],
        (far_rows, far_own, interp, *others),
        [SMEM] + [VMEM] * (2 + len(others)),
        [
            pltpu.VMEM((n_blocks, n_skel, 4 * dim), BF16),
            pltpu.VMEM((n_blocks, n_skel, 2 * LANES), BF16),
            pltpu.VMEM((leaves, n_skel, 4 * dim), BF16),
        ],
        flops=leaves * 8 * 2 * n_skel * n_skel * 256 * 3,
    )
    (out,) = call(
        functools.partial(last_kernel, devs, pair, leaf, scale),
        [f32(devs * 2 * pair, LANES)],
        (lists, counts, pos, targets, *blocks[half // 2], acc, own_sum, far_part, theirs[rows // 2 :]),
        [SMEM] * 3 + [VMEM] * 7,
        [pltpu.VMEM((2 * rows + leaf, LANES), F32)]
        + tiles(leaves)
        + [
            pltpu.VMEM((devs, LANES), jnp.int32),
            pltpu.SMEM((devs, LANES), jnp.int32),
            pltpu.SemaphoreType.DMA,
        ],
        flops=2 * leaves * per_leaf,
    )
    returned = lax.all_to_all(out.reshape(devs, 2 * pair, LANES), JOINT, 0, 0, tiled=True)
    (final,) = call(
        functools.partial(final_kernel, pair, n_inner),
        [f32(rows, LANES)],
        (returned.reshape(devs * 2 * pair, LANES), code),
        [VMEM, SMEM],
        [pltpu.VMEM((rows, LANES), F32)],
    )
    return final


def solution(mesh):
    row = P(JOINT, None)
    in_specs = (row, row, row, P(JOINT), P(), P(), row)
    return jax.shard_map(shards, mesh=mesh, in_specs=in_specs, out_specs=row, check_vma=False)
```

```python
import functools
import math

import jax
import jax.numpy as jnp
from jax import lax
from jax.experimental import pallas as pl
from jax.experimental.pallas import tpu as pltpu
from jax.sharding import PartitionSpec as P


F32 = jnp.float32
BF16 = jnp.bfloat16
LANES = 128
JOINT = ("outer", "inner")
VMEM = pl.BlockSpec(memory_space=pltpu.VMEM)
SMEM = pl.BlockSpec(memory_space=pltpu.SMEM)
HBM = pl.BlockSpec(memory_space=pltpu.HBM)


def call(body, outs, args, in_specs, scratch=(), out_specs=None, flops=0, room=3):
    nbytes = sum(a.size * a.dtype.itemsize for a in (*args, *outs))
    held = sum(math.prod(s.shape) * jnp.dtype(s.dtype).itemsize for s in scratch if getattr(s, "memory_space", None) == pltpu.VMEM)
    limit = min(60 << 20, nbytes + held + (room << 20))
    return pl.pallas_call(
        body,
        out_shape=outs,
        in_specs=in_specs,
        out_specs=out_specs or [VMEM] * len(outs),
        scratch_shapes=list(scratch),
        compiler_params=pltpu.CompilerParams(vmem_limit_bytes=limit),
        cost_estimate=pl.CostEstimate(flops=flops, bytes_accessed=nbytes, transcendentals=0),
    )(*args)


def split(x):
    hi = x.astype(BF16)
    return hi, (x - hi.astype(F32)).astype(BF16)


def pack(rows, dim):
    half = rows.shape[0] // 2
    return jnp.concatenate([rows[:half, :dim], rows[half:, :dim]], axis=1)


def exponent_side(packed, dim, scale, is_target):
    lane = lax.broadcasted_iota(jnp.int32, packed.shape, 1)
    first = lane < dim
    turned = jnp.concatenate([packed[:, dim:], packed[:, :dim]], axis=1)
    at = dim + (0 if is_target else 3)
    ones = jnp.where((lane >= dim) & (lane < dim + 6), 1.0, 0.0)
    blocks = []
    for x in (jnp.where(first, packed, turned), jnp.where(first, turned, packed)):
        n = jnp.sum(x * x, axis=1, keepdims=True) * (-0.5 * scale)
        norms = jnp.where(lane == at, n, ones)
        for j in (1, 2):
            n = n - n.astype(BF16).astype(F32)
            norms = jnp.where(lane == at + j, n, norms)
        if is_target:
            x = x * (2.0 * scale)
        low = x - x.astype(BF16).astype(F32)
        if is_target:
            head, tail = jnp.where(first, x, low), jnp.where(first, x, norms)
        else:
            head, tail = x, jnp.where(first, low, norms)
        blocks.append(jnp.concatenate([head, tail], axis=1).astype(BF16))
    return blocks


def load_points(ref, pitch, skip, base, out, scale, is_target):
    count = ref.shape[0] // pitch
    size = out.shape[1] // 2
    step = size
    parts = size // step

    def body(i, carry):
        g, c = div_mod(i, parts)
        at = pl.multiple_of(g * pitch + skip + c * step, 8)
        blocks = exponent_side(ref[pl.ds(at, step), :], LANES // 2, scale, is_target)
        for j, value in enumerate(blocks):
            out[base + g, pl.ds(pl.multiple_of(j * size + c * step, step), step), :] = value
        return carry

    lax.fori_loop(0, count * parts, body, 0)


def load_charges(ref, pitch, base, out):
    count = ref.shape[0] // pitch
    step = 256
    parts = out.shape[1] // step

    def body(i, carry):
        g, c = div_mod(i, parts)
        at = pl.multiple_of(g * pitch + c * step, 8)
        hi, lo = split(ref[pl.ds(at, step), :])
        rows = pl.ds(pl.multiple_of(c * step, step), step)
        out[base + g, rows, :LANES] = hi
        out[base + g, rows, LANES:] = lo
        return carry

    lax.fori_loop(0, count * parts, body, 0)


def charge_side(c):
    hi, lo = split(c)
    return jnp.concatenate([hi, lo], axis=1)


def nt_dot(a, b):
    return lax.dot_general(a, b, (((1,), (1,)), ((), ())), preferred_element_type=F32)


def tn_dot(a, b):
    return lax.dot_general(a, b, (((0,), (0,)), ((), ())), preferred_element_type=F32)


def fold(p):
    half = p.shape[1] // 2
    return p[:, :half] + p[:, half:]


def tile_product(target, source, charge):
    k = jnp.exp2(nt_dot(target, source))
    hi, lo = split(k)
    return fold(
        jnp.dot(hi, charge, preferred_element_type=F32)
        + jnp.dot(lo, charge, preferred_element_type=F32)
    )


def div_mod(x, n):
    if n & (n - 1) == 0:
        return lax.shift_right_logical(x, jnp.int32(n.bit_length() - 1)), x & (n - 1)
    q = lax.div(x, jnp.int32(n))
    return q, x - q * n


UNROLL = 64


def rows_loop(count, body):
    def step(i, carry):
        line, part = div_mod(i, LANES // UNROLL)
        for u in range(UNROLL):
            body(i * UNROLL + u, line, part * UNROLL + u)
        return carry

    lax.fori_loop(0, count // UNROLL, step, 0)


def send_kernel(devs, pair, block, order_hbm, pts_hbm, chg_hbm, send_ref, code_ref, ptmp, prow, order_ref, pts_ref, chg_ref, idx_v, idx_s, sem, sems):
    loads = [
        pltpu.make_async_copy(a, b, sems.at[i])
        for i, (a, b) in enumerate(((order_hbm, order_ref), (chg_hbm, chg_ref), (pts_hbm, pts_ref)))
    ]
    for load in loads:
        load.start()
    loads[0].wait()
    rows = chg_ref.shape[0]
    dim = pts_ref.shape[0]
    lines = rows // LANES
    dest, slot = div_mod(order_ref[...], rows)
    sub = lax.broadcasted_iota(jnp.int32, (devs, LANES), 0)
    hot = [jnp.where(dest[r : r + 1, :] == sub, 1.0, 0.0) for r in range(lines)]
    ki = lax.broadcasted_iota(jnp.int32, (LANES, 2 * LANES), 0)
    ji = lax.broadcasted_iota(jnp.int32, (LANES, 2 * LANES), 1)
    tri = jnp.where((ki < ji) | (ji >= LANES), 1.0, 0.0).astype(BF16)
    pre = jnp.dot(jnp.concatenate([h.astype(BF16) for h in hot], axis=0), tri, preferred_element_type=F32)
    base = jnp.zeros((devs, LANES), F32)
    ranks = []
    for r in range(lines):
        part = pre[r * devs : (r + 1) * devs]
        ranks.append(jnp.sum(hot[r] * (part[:, :LANES] + base), axis=0, keepdims=True))
        base = base + part[:, LANES:]
    rank_f = jnp.concatenate(ranks, axis=0)
    rank = rank_f.astype(jnp.int32)
    idx_v[...] = dest * block + rank
    copy = pltpu.make_async_copy(idx_v, idx_s, sem)
    copy.start()
    code_ref[...] = dest * pair + rank
    psub = lax.broadcasted_iota(jnp.int32, (pair, LANES), 0)
    s_hi = lax.shift_right_logical(slot, 8).astype(F32)
    s_lo = (slot & 255).astype(F32)
    left, right = [], []
    for r in range(lines):
        left.append(
            jnp.concatenate([hot[r] * s_hi[r : r + 1, :], hot[r] * s_lo[r : r + 1, :]], axis=0).astype(BF16)
        )
        right.append(jnp.where(rank[r : r + 1, :] == psub, 1.0, 0.0).astype(BF16))
    both = nt_dot(jnp.concatenate(left, axis=1), jnp.concatenate(right, axis=1))
    table = both[:devs] * 256.0 + both[devs:]
    if pair < LANES:
        table = jnp.concatenate([table, jnp.zeros((devs, LANES - pair), F32)], axis=1)
    loads[2].wait()
    for c in range(0, rows, 256):
        prow[c : c + 256, :dim] = pts_ref[:, c : c + 256].T
    loads[1].wait()
    copy.wait()

    def move(n, line, lane):
        j = idx_s[line, lane]
        send_ref[pl.ds(j, 1), :] = chg_ref[pl.ds(n, 1), :]
        ptmp[pl.ds(j, 1), :] = prow[pl.ds(n, 1), :]

    rows_loop(rows, move)
    half = pair // 2
    for d in range(devs):
        send_ref[d * block + pair : d * block + pair + half, :] = pack(
            ptmp[d * block : d * block + pair, :], dim
        )
        send_ref[d * block + pair + half : (d + 1) * block, :] = jnp.broadcast_to(
            table[d : d + 1, :], (block - pair - half, LANES)
        )


def place_kernel(devs, pair, block, leaf, dim, recv_ref, low_ref, high_ref, pts_ref, exch_ref, pos_ref, rolled, chg, pos_s, sem):
    half = pair // 2
    rows = pts_ref.shape[0]
    leaves = rows // leaf
    line = leaf + leaf // 2
    table = jnp.concatenate(
        [recv_ref[d * block + pair + half : d * block + pair + half + 1, :] for d in range(devs)], axis=0
    )
    pos_ref[...] = table.astype(jnp.int32)
    copy = pltpu.make_async_copy(pos_ref, pos_s, sem)
    copy.start()
    exch_ref[rows // 2 :, :] = table
    for d in range(devs):
        part = recv_ref[d * block + pair : d * block + pair + half, :]
        rolled[d * half : (d + 1) * half, :] = jnp.concatenate([part[:, dim:], part[:, :dim]], axis=1)
    copy.wait()

    def per_source(d, carry):
        for j in range(pair):
            p = pos_s[d, j]
            chg[pl.ds(p, 1), :] = recv_ref[pl.ds(d * block + j, 1), :]
            if j < half:
                pts_ref[pl.ds(p, 1), :] = recv_ref[pl.ds(d * block + pair + j, 1), :]
            else:
                pts_ref[pl.ds(p, 1), :] = rolled[pl.ds(d * half + j - half, 1), :]
        return carry

    lax.fori_loop(0, devs, per_source, 0)
    for g in range(leaves):
        packed = pack(pts_ref[g * leaf : (g + 1) * leaf, :], dim)
        ref, at = (low_ref, g * line) if g < leaves // 2 else (high_ref, (g - leaves // 2) * line)
        ref[at : at + leaf, :] = chg[g * leaf : (g + 1) * leaf, :]
        ref[at + leaf : at + line, :] = packed
        exch_ref[g * (leaf // 2) : (g + 1) * (leaf // 2), :] = packed


def skeleton_kernel(leaf, dim, low_ref, high_ref, pts_ref, interp_ref, skel_ref, far_ref, stmp):
    leaves, skel = skel_ref.shape
    line = leaf + leaf // 2
    fline = skel + skel // 2

    for g in range(leaves):

        def move(n, line, lane, g=g):
            stmp[pl.ds(g * skel + n, 1), :] = pts_ref[pl.ds(g * leaf + skel_ref[g, n], 1), :]

        rows_loop(skel, move)
    for g in range(leaves):
        hi, lo = split(interp_ref[g * leaf : (g + 1) * leaf, :])
        ref, at = (low_ref, g * line) if g < leaves // 2 else (high_ref, (g - leaves // 2) * line)
        charge = charge_side(ref[at : at + leaf, :])
        far_ref[g * fline : g * fline + skel, :] = fold(tn_dot(hi, charge) + tn_dot(lo, charge))
        far_ref[g * fline + skel : (g + 1) * fline, :] = pack(stmp[g * skel : (g + 1) * skel, :], dim)


def far_kernel(skel, scale, n_inner, blocks, far_rows_ref, own_hbm, interp_hbm, *rest):
    hbm, (out_ref, src, chg, tgt), bufs, sems = rest[:blocks], rest[blocks : blocks + 4], rest[blocks + 4 : -1], rest[-1]
    own, *refs, interp = bufs
    copies = start_loads([own_hbm, *hbm, interp_hbm], bufs, sems)
    leaves, fars = far_rows_ref.shape
    leaf = interp_hbm.shape[0] // leaves
    fline = skel + skel // 2
    outer = lax.axis_index("outer")
    copies[0].wait()
    load_points(own, fline, skel, 0, tgt, scale, True)
    for b in range(blocks):
        copies[b + 1].wait()
        load_points(refs[b], fline, skel, b * leaves, src, scale, False)
        load_charges(refs[b], fline, b * leaves, chg)
    copies[-1].wait()

    for g in range(leaves):
        q = jnp.zeros((skel, LANES), F32)
        for k in range(0, fars, 2):
            ats = []
            for j in range(k, min(k + 2, fars)):
                device, local = div_mod(far_rows_ref[g, j], leaves)
                ats.append(((device // n_inner) ^ outer) * leaves - leaves + local)
            q = q + tile_product(
                tgt[g],
                jnp.concatenate([src[at] for at in ats], axis=0),
                jnp.concatenate([chg[at] for at in ats], axis=0),
            )
        qq = charge_side(q)
        hi, lo = split(interp[g * leaf : (g + 1) * leaf, :])
        out_ref[g * leaf : (g + 1) * leaf, :] = fold(
            jnp.dot(hi, qq, preferred_element_type=F32) + jnp.dot(lo, qq, preferred_element_type=F32)
        )


def target_kernel(leaf, scale, own_ref, theirs_ref, out_ref):
    leaves = own_ref.shape[0]
    out_ref[:leaves] = own_ref[...]
    load_points(theirs_ref.at[: leaves * leaf // 2], leaf // 2, 0, leaves, out_ref, scale, True)


CODE = 1024
GROUP = 4


def list_kernel(leaves, n_inner, near_ref, list_ref, count_ref):
    half = n_inner // 2
    cut = leaves // 2
    n_near = near_ref.shape[1]
    inner = lax.axis_index("inner")
    for row in range(4):
        count_ref[row] = 0

    def add(row, code):
        n = count_ref[row]
        list_ref[row, n] = code
        count_ref[row] = n + 1

    def entry(e, carry):
        row, k = div_mod(e, n_near)
        device, local = div_mod(near_ref[row, k], leaves)
        away = (device & (n_inner - 1)) ^ inner
        last = away == half - 1
        high = local >= cut
        theirs = row >= leaves
        which = jnp.where(last, jnp.where(high, 3, 2), jnp.where(theirs, 1, 0))
        source = jnp.where(last, jnp.where(high, local - cut, local), away * leaves + local)

        @pl.when((away < half) & ((away != 0) | theirs))
        def _():
            add(which, row * CODE + source)

        return carry

    lax.fori_loop(0, 2 * leaves * n_near, entry, 0)
    for row in range(4):
        for _ in range(GROUP - 1):

            @pl.when(count_ref[row] % GROUP != 0)
            def _():
                add(row, (leaves if row == 0 else 2 * leaves) * CODE)


def start_loads(hbm_refs, bufs, sems):
    copies = [pltpu.make_async_copy(a, b, sems.at[i]) for i, (a, b) in enumerate(zip(hbm_refs, bufs))]
    for copy in copies:
        copy.start()
    return copies


def load_sources(leaf, scale, refs, src, chg, at=0, copies=None):
    line = leaf + leaf // 2
    for i, ref in enumerate(refs):
        if copies:
            copies[i].wait()
        load_points(ref, line, leaf, at, src, scale, False)
        load_charges(ref, line, at, chg)
        at += ref.shape[0] // line


def leaf_rows(t, c, leaf, step):
    return pl.ds(pl.multiple_of(t * leaf + c, step), step)


def self_kernel(leaf, scale, own_ref, low_ref, high_ref, acc_ref, src, chg, tgt):
    leaves = src.shape[0]
    load_sources(leaf, scale, (low_ref, high_ref), src, chg)
    load_points(own_ref.at[: leaves * leaf // 2], leaf // 2, 0, 0, tgt, scale, True)
    step = leaf // 2

    def entry(e, carry):
        for t in (2 * e, 2 * e + 1):
            for c in range(0, leaf, step):
                acc_ref[leaf_rows(t, c, leaf, step), :] = tile_product(
                    tgt[t, c : c + step, :], src[t], chg[t]
                )
        return carry

    lax.fori_loop(0, leaves // 2, entry, 0)


def add_listed(leaf, row, list_ref, count_ref, tgt, src, chg, acc):
    step = leaf // 2

    def entry(e, carry):
        for u in range(GROUP):
            t, at = div_mod(list_ref[row, e * GROUP + u], CODE)
            x = jnp.minimum(t, tgt.shape[0] - 1)
            for c in range(0, leaf, step):
                acc[leaf_rows(t, c, leaf, step), :] += tile_product(
                    tgt[x, c : c + step, :], src[at], chg[at]
                )
        return carry

    lax.fori_loop(0, lax.shift_right_logical(count_ref[row], jnp.int32(GROUP.bit_length() - 1)), entry, 0)


def own_near_kernel(leaf, scale, list_ref, count_ref, tgt_ref, src_ref, chg_ref, *rest):
    n = (len(rest) - 4) // 2
    sources, (acc_ref, src, chg), bufs, sems = rest[:n], rest[n : n + 3], rest[n + 3 : -1], rest[-1]
    copies = start_loads(sources, bufs, sems)
    leaves = src_ref.shape[0]
    src[:leaves] = src_ref[...]
    chg[:leaves] = chg_ref[...]
    acc_ref[...] = jnp.zeros_like(acc_ref)
    load_sources(leaf, scale, bufs, src, chg, leaves, copies)
    add_listed(leaf, 0, list_ref, count_ref, tgt_ref, src, chg, acc_ref)


def near_kernel(leaf, scale, list_ref, count_ref, tgt_ref, src_ref, chg_ref, low_hbm, own_ref, acc_ref, src, chg, low, sems):
    rows = own_ref.shape[0] - leaf
    copies = start_loads([low_hbm], [low], sems)
    acc_ref[:rows, :] = own_ref[:rows, :]
    acc_ref[rows:, :] = jnp.zeros((acc_ref.shape[0] - rows, LANES), F32)
    add_listed(leaf, 1, list_ref, count_ref, tgt_ref, src_ref, chg_ref, acc_ref)
    load_sources(leaf, scale, (low,), src, chg, 0, copies)
    add_listed(leaf, 2, list_ref, count_ref, tgt_ref, src, chg, acc_ref)


def last_kernel(devs, pair, leaf, scale, list_ref, count_ref, pos_ref, tgt_ref, piece_hbm, old_ref, self_ref, far_ref, theirs_hbm, out_ref, acc, src, chg, opos_v, opos_s, sem, held, opos_f, sems):
    rows = far_ref.shape[0]
    table = theirs_hbm.at[pl.ds(rows // 2, devs), :]
    copies = start_loads([piece_hbm, table], [held, opos_f], sems)
    copies[1].wait()
    opos_v[...] = opos_f[...].astype(jnp.int32)
    copy = pltpu.make_async_copy(opos_v, opos_s, sem)
    copy.start()
    acc[:rows, :] = old_ref[:rows, :] + (self_ref[...] + far_ref[...])
    acc[rows:, :] = old_ref[rows:, :]
    load_sources(leaf, scale, (held,), src, chg, 0, copies)
    add_listed(leaf, 3, list_ref, count_ref, tgt_ref, src, chg, acc)
    copy.wait()

    def per_source(d, carry):
        for j in range(pair):
            out_ref[pl.ds(d * 2 * pair + j, 1), :] = acc[pl.ds(pos_ref[d, j], 1), :]
            out_ref[pl.ds(d * 2 * pair + pair + j, 1), :] = acc[pl.ds(rows + opos_s[d, j], 1), :]
        return carry

    lax.fori_loop(0, devs, per_source, 0)


def final_kernel(pair, n_inner, ret_ref, code_ref, out_hbm, both, out, sems):
    devs = both.shape[0] // pair
    for d in range(devs):
        other = d ^ (n_inner // 2)
        both[d * pair : (d + 1) * pair, :] = (
            ret_ref[2 * d * pair : (2 * d + 1) * pair, :]
            + ret_ref[(2 * other + 1) * pair : (2 * other + 2) * pair, :]
        )

    parts = sems.shape[0]
    size = out.shape[0] // parts
    steps = size // UNROLL
    copies = []
    for p in range(parts):

        def step(i, carry):
            line, part = div_mod(i, LANES // UNROLL)
            for u in range(UNROLL):
                row = both[pl.ds(code_ref[line, part * UNROLL + u], 1), :]
                out[pl.ds(i * UNROLL + u, 1), :] = row
            return carry

        lax.fori_loop(p * steps, (p + 1) * steps, step, 0)
        rows = pl.ds(p * size, size)
        copies.append(pltpu.make_async_copy(out.at[rows, :], out_hbm.at[rows, :], sems.at[p]))
        copies[-1].start()
    for copy in copies:
        copy.wait()


def shards(points, charges, interp, order, near, far, skel):
    n_inner = lax.axis_size("inner")
    n_outer = lax.axis_size("outer")
    devs = n_inner * n_outer
    rows, dim = points.shape
    leaves, n_skel = skel.shape
    leaf = rows // leaves
    line = leaf + leaf // 2
    fline = n_skel + n_skel // 2
    pair = rows // devs
    block = pair + pair // 2 + 8
    scale = (4.0 / dim) * math.log2(math.e)
    outer = lax.axis_index("outer")
    inner = lax.axis_index("inner")
    me = outer * n_inner + inner
    half = n_inner // 2
    partner = outer * n_inner + (inner ^ half)

    def f32(*shape):
        return jax.ShapeDtypeStruct(shape, F32)

    def i32(*shape):
        return jax.ShapeDtypeStruct(shape, jnp.int32)

    def near_of(device):
        return lax.dynamic_slice_in_dim(near, device * leaves, leaves, 0)

    near_rows = jnp.concatenate([near_of(me), near_of(partner)], axis=0)
    far_rows = lax.dynamic_slice_in_dim(far, me * leaves, leaves, 0)

    send, code = call(
        functools.partial(send_kernel, devs, pair, block),
        [f32(devs * block, LANES), i32(rows // LANES, LANES)],
        (order.reshape(rows // LANES, LANES), points.T, charges),
        [HBM] * 3,
        [
            pltpu.VMEM((devs * block, LANES), F32),
            pltpu.VMEM((rows, LANES), F32),
            pltpu.VMEM((rows // LANES, LANES), jnp.int32),
            pltpu.VMEM((dim, rows), F32),
            pltpu.VMEM((rows, LANES), F32),
            pltpu.VMEM((rows // LANES, LANES), jnp.int32),
            pltpu.SMEM((rows // LANES, LANES), jnp.int32),
            pltpu.SemaphoreType.DMA,
            pltpu.SemaphoreType.DMA((3,)),
        ],
        room=60,
    )
    recv = lax.all_to_all(send.reshape(devs, block, LANES), JOINT, 0, 0, tiled=True)
    piece = leaves // 2 * line
    own_low, own_high, pts, exch, pos = call(
        functools.partial(place_kernel, devs, pair, block, leaf, dim),
        [f32(piece, LANES), f32(piece, LANES), f32(rows, LANES), f32(rows // 2 + devs, LANES), i32(devs, LANES)],
        (recv.reshape(devs * block, LANES),),
        [VMEM],
        [
            pltpu.VMEM((devs * pair // 2, LANES), F32),
            pltpu.VMEM((rows, LANES), F32),
            pltpu.SMEM((devs, LANES), jnp.int32),
            pltpu.SemaphoreType.DMA,
        ],
    )

    def swap(x, bit):
        return lax.ppermute(x, "inner", [(i, i ^ bit) for i in range(n_inner)])

    blocks = {0: (own_low, own_high)}
    for r in sorted(range(1, half), key=lambda r: (r.bit_count(), r)):
        down, up = r & -r, 1 << (r.bit_length() - 1)
        by_low = 0 if r == down else r ^ down
        by_high = 0 if r == up else r ^ up
        blocks[r] = (swap(blocks[by_low][0], r ^ by_low), swap(blocks[by_high][1], r ^ by_high))
    theirs = swap(exch, half)

    (far_own,) = call(
        functools.partial(skeleton_kernel, leaf, dim),
        [f32(leaves * fline, LANES)],
        (own_low, own_high, pts, interp, skel),
        [VMEM, VMEM, VMEM, VMEM, SMEM],
        [pltpu.VMEM((leaves * n_skel, LANES), F32)],
        flops=2 * rows * n_skel * 3 * 128,
    )
    held = {0: far_own}
    bit = n_outer // 2
    while bit:
        perm = [(o, o ^ bit) for o in range(n_outer)]
        got = {}
        for r, v in held.items():
            got[r ^ bit] = lax.ppermute(v, "outer", perm)
        held.update(got)
        bit //= 2

    lists, counts = call(
        functools.partial(list_kernel, leaves, n_inner),
        [i32(4, 2 * leaves * near.shape[1]), i32(4)],
        (near_rows,),
        [SMEM],
        out_specs=[SMEM, SMEM],
    )

    def tiles(count):
        return [
            pltpu.VMEM((count, leaf, 4 * dim), BF16),
            pltpu.VMEM((count, leaf, 2 * LANES), BF16),
        ]

    per_leaf = 2 * leaf * leaf * 256 * 3
    own_sum, own_src, own_chg, own_tgt = call(
        functools.partial(self_kernel, leaf, scale),
        [f32(rows, LANES)] + [jax.ShapeDtypeStruct((leaves, leaf, 4 * dim), BF16)] * 3,
        (exch, own_low, own_high),
        [VMEM] * 3,
        flops=leaves * per_leaf,
    )
    (targets,) = call(
        functools.partial(target_kernel, leaf, scale),
        [jax.ShapeDtypeStruct((2 * leaves, leaf, 4 * dim), BF16)],
        (own_tgt, theirs),
        [VMEM] * 2,
        flops=1 << 20,
    )
    sources = [piece for r in range(1, half - 1) for piece in blocks[r]]
    held_tiles = [jax.ShapeDtypeStruct(((half - 1) * leaves, leaf, 4 * dim), BF16)] * 2
    acc, src, chg = call(
        functools.partial(own_near_kernel, leaf, scale),
        [f32(rows + leaf, LANES)] + held_tiles,
        (lists, counts, own_tgt, own_src, own_chg, *sources),
        [SMEM, SMEM] + [VMEM] * 3 + [HBM] * len(sources),
        [pltpu.VMEM((piece, LANES), F32)] * len(sources) + [pltpu.SemaphoreType.DMA((len(sources),))],
        flops=(half - 2) * leaves * per_leaf,
    )
    (acc,) = call(
        functools.partial(near_kernel, leaf, scale),
        [f32(2 * rows + leaf, LANES)],
        (lists, counts, targets, src, chg, blocks[half - 1][0], acc),
        [SMEM, SMEM] + [VMEM] * 3 + [HBM, VMEM],
        tiles(leaves // 2) + [pltpu.VMEM((piece, LANES), F32), pltpu.SemaphoreType.DMA((1,))],
        flops=half * leaves * per_leaf,
    )
    others = [held[r] for r in range(1, n_outer)]
    n_blocks = len(others) * leaves
    (far_part,) = call(
        functools.partial(far_kernel, n_skel, scale, n_inner, len(others)),
        [f32(rows, LANES)],
        (far_rows, far_own, interp, *others),
        [SMEM] + [HBM] * (2 + len(others)),
        [
            pltpu.VMEM((n_blocks, n_skel, 4 * dim), BF16),
            pltpu.VMEM((n_blocks, n_skel, 2 * LANES), BF16),
            pltpu.VMEM((leaves, n_skel, 4 * dim), BF16),
        ]
        + [pltpu.VMEM((leaves * fline, LANES), F32)] * (1 + len(others))
        + [pltpu.VMEM(interp.shape, F32), pltpu.SemaphoreType.DMA((2 + len(others),))],
        flops=leaves * 8 * 2 * n_skel * n_skel * 256 * 3,
    )
    (out,) = call(
        functools.partial(last_kernel, devs, pair, leaf, scale),
        [f32(devs * 2 * pair, LANES)],
        (lists, counts, pos, targets, blocks[half - 1][1], acc, own_sum, far_part, theirs),
        [SMEM] * 3 + [VMEM, HBM] + [VMEM] * 3 + [HBM],
        [pltpu.VMEM((2 * rows + leaf, LANES), F32)]
        + tiles(leaves // 2)
        + [
            pltpu.VMEM((devs, LANES), jnp.int32),
            pltpu.SMEM((devs, LANES), jnp.int32),
            pltpu.SemaphoreType.DMA,
            pltpu.VMEM((piece, LANES), F32),
            pltpu.VMEM((devs, LANES), F32),
            pltpu.SemaphoreType.DMA((2,)),
        ],
        flops=2 * leaves * per_leaf,
    )
    returned = lax.all_to_all(out.reshape(devs, 2 * pair, LANES), JOINT, 0, 0, tiled=True)
    (final,) = call(
        functools.partial(final_kernel, pair, n_inner),
        [f32(rows, LANES)],
        (returned.reshape(devs * 2 * pair, LANES), code),
        [VMEM, SMEM],
        [pltpu.VMEM((rows, LANES), F32), pltpu.VMEM((rows, LANES), F32), pltpu.SemaphoreType.DMA((4,))],
        out_specs=[HBM],
    )
    return final


def solution(mesh):
    row = P(JOINT, None)
    in_specs = (row, row, row, P(JOINT), P(), P(), row)
    return jax.shard_map(shards, mesh=mesh, in_specs=in_specs, out_specs=row, check_vma=False)
```

```python
import functools
import math

import jax
import jax.numpy as jnp
from jax import lax
from jax.experimental import pallas as pl
from jax.experimental.pallas import tpu as pltpu
from jax.sharding import PartitionSpec as P


F32 = jnp.float32
BF16 = jnp.bfloat16
LANES = 128
JOINT = ("outer", "inner")
VMEM = pl.BlockSpec(memory_space=pltpu.VMEM)
SMEM = pl.BlockSpec(memory_space=pltpu.SMEM)
HBM = pl.BlockSpec(memory_space=pltpu.HBM)


def call(body, outs, args, in_specs, scratch=(), out_specs=None, flops=0, room=3):
    nbytes = sum(a.size * a.dtype.itemsize for a in (*args, *outs))
    held = sum(math.prod(s.shape) * jnp.dtype(s.dtype).itemsize for s in scratch if getattr(s, "memory_space", None) == pltpu.VMEM)
    limit = min(60 << 20, nbytes + held + (room << 20))
    return pl.pallas_call(
        body,
        out_shape=outs,
        in_specs=in_specs,
        out_specs=out_specs or [VMEM] * len(outs),
        scratch_shapes=list(scratch),
        compiler_params=pltpu.CompilerParams(vmem_limit_bytes=limit),
        cost_estimate=pl.CostEstimate(flops=flops, bytes_accessed=nbytes, transcendentals=0),
    )(*args)


def split(x):
    hi = x.astype(BF16)
    return hi, (x - hi.astype(F32)).astype(BF16)


def pack(rows, dim):
    half = rows.shape[0] // 2
    return jnp.concatenate([rows[:half, :dim], rows[half:, :dim]], axis=1)


def exponent_side(packed, dim, scale, is_target):
    lane = lax.broadcasted_iota(jnp.int32, packed.shape, 1)
    first = lane < dim
    turned = jnp.concatenate([packed[:, dim:], packed[:, :dim]], axis=1)
    at = dim + (0 if is_target else 3)
    ones = jnp.where((lane >= dim) & (lane < dim + 6), 1.0, 0.0)
    blocks = []
    for x in (jnp.where(first, packed, turned), jnp.where(first, turned, packed)):
        n = jnp.sum(x * x, axis=1, keepdims=True) * (-0.5 * scale)
        norms = jnp.where(lane == at, n, ones)
        for j in (1, 2):
            n = n - n.astype(BF16).astype(F32)
            norms = jnp.where(lane == at + j, n, norms)
        if is_target:
            x = x * (2.0 * scale)
        low = x - x.astype(BF16).astype(F32)
        if is_target:
            head, tail = jnp.where(first, x, low), jnp.where(first, x, norms)
        else:
            head, tail = x, jnp.where(first, low, norms)
        blocks.append(jnp.concatenate([head, tail], axis=1).astype(BF16))
    return blocks


def load_points(ref, pitch, skip, base, out, scale, is_target):
    count = ref.shape[0] // pitch
    size = out.shape[1] // 2
    step = size
    parts = size // step

    def body(i, carry):
        g, c = div_mod(i, parts)
        at = pl.multiple_of(g * pitch + skip + c * step, 8)
        blocks = exponent_side(ref[pl.ds(at, step), :], LANES // 2, scale, is_target)
        for j, value in enumerate(blocks):
            out[base + g, pl.ds(pl.multiple_of(j * size + c * step, step), step), :] = value
        return carry

    lax.fori_loop(0, count * parts, body, 0)


def load_charges(ref, pitch, base, out):
    count = ref.shape[0] // pitch
    step = 256
    parts = out.shape[1] // step

    def body(i, carry):
        g, c = div_mod(i, parts)
        at = pl.multiple_of(g * pitch + c * step, 8)
        hi, lo = split(ref[pl.ds(at, step), :])
        rows = pl.ds(pl.multiple_of(c * step, step), step)
        out[base + g, rows, :LANES] = hi
        out[base + g, rows, LANES:] = lo
        return carry

    lax.fori_loop(0, count * parts, body, 0)


def charge_side(c):
    hi, lo = split(c)
    return jnp.concatenate([hi, lo], axis=1)


def nt_dot(a, b):
    return lax.dot_general(a, b, (((1,), (1,)), ((), ())), preferred_element_type=F32)


def tn_dot(a, b):
    return lax.dot_general(a, b, (((0,), (0,)), ((), ())), preferred_element_type=F32)


def fold(p):
    half = p.shape[1] // 2
    return p[:, :half] + p[:, half:]


def tile_product(target, source, charge):
    k = jnp.exp2(nt_dot(target, source))
    hi, lo = split(k)
    return fold(
        jnp.dot(hi, charge, preferred_element_type=F32)
        + jnp.dot(lo, charge, preferred_element_type=F32)
    )


def div_mod(x, n):
    if n & (n - 1) == 0:
        return lax.shift_right_logical(x, jnp.int32(n.bit_length() - 1)), x & (n - 1)
    q = lax.div(x, jnp.int32(n))
    return q, x - q * n


def rows_loop(count, body):
    def step(line, carry):
        for lane in range(LANES):
            body(line * LANES + lane, line, lane)
        return carry

    lax.fori_loop(0, count // LANES, step, 0)


def send_kernel(devs, pair, block, order_hbm, pts_hbm, chg_hbm, send_ref, code_ref, ptmp, prow, order_ref, pts_ref, chg_ref, idx_v, idx_s, sem, sems):
    loads = [
        pltpu.make_async_copy(a, b, sems.at[i])
        for i, (a, b) in enumerate(((order_hbm, order_ref), (chg_hbm, chg_ref), (pts_hbm, pts_ref)))
    ]
    for load in loads:
        load.start()
    loads[0].wait()
    rows = chg_ref.shape[0]
    dim = pts_ref.shape[0]
    lines = rows // LANES
    dest, slot = div_mod(order_ref[...], rows)
    sub = lax.broadcasted_iota(jnp.int32, (devs, LANES), 0)
    hot = [jnp.where(dest[r : r + 1, :] == sub, 1.0, 0.0) for r in range(lines)]
    ki = lax.broadcasted_iota(jnp.int32, (LANES, 2 * LANES), 0)
    ji = lax.broadcasted_iota(jnp.int32, (LANES, 2 * LANES), 1)
    tri = jnp.where((ki < ji) | (ji >= LANES), 1.0, 0.0).astype(BF16)
    pre = jnp.dot(jnp.concatenate([h.astype(BF16) for h in hot], axis=0), tri, preferred_element_type=F32)
    base = jnp.zeros((devs, LANES), F32)
    ranks = []
    for r in range(lines):
        part = pre[r * devs : (r + 1) * devs]
        ranks.append(jnp.sum(hot[r] * (part[:, :LANES] + base), axis=0, keepdims=True))
        base = base + part[:, LANES:]
    rank_f = jnp.concatenate(ranks, axis=0)
    rank = rank_f.astype(jnp.int32)
    idx_v[...] = dest * block + rank
    copy = pltpu.make_async_copy(idx_v, idx_s, sem)
    copy.start()
    code_ref[...] = dest * pair + rank
    psub = lax.broadcasted_iota(jnp.int32, (pair, LANES), 0)
    s_hi = lax.shift_right_logical(slot, 8).astype(F32)
    s_lo = (slot & 255).astype(F32)
    left, right = [], []
    for r in range(lines):
        left.append(
            jnp.concatenate([hot[r] * s_hi[r : r + 1, :], hot[r] * s_lo[r : r + 1, :]], axis=0).astype(BF16)
        )
        right.append(jnp.where(rank[r : r + 1, :] == psub, 1.0, 0.0).astype(BF16))
    both = nt_dot(jnp.concatenate(left, axis=1), jnp.concatenate(right, axis=1))
    table = both[:devs] * 256.0 + both[devs:]
    if pair < LANES:
        table = jnp.concatenate([table, jnp.zeros((devs, LANES - pair), F32)], axis=1)
    loads[2].wait()
    for c in range(0, rows, 256):
        prow[c : c + 256, :dim] = pts_ref[:, c : c + 256].T
    loads[1].wait()
    copy.wait()

    def move(n, line, lane):
        j = idx_s[line, lane]
        send_ref[pl.ds(j, 1), :] = chg_ref[pl.ds(n, 1), :]
        ptmp[pl.ds(j, 1), :] = prow[pl.ds(n, 1), :]

    rows_loop(rows, move)
    half = pair // 2
    for d in range(devs):
        send_ref[d * block + pair : d * block + pair + half, :] = pack(
            ptmp[d * block : d * block + pair, :], dim
        )
        send_ref[d * block + pair + half : (d + 1) * block, :] = jnp.broadcast_to(
            table[d : d + 1, :], (block - pair - half, LANES)
        )


def place_kernel(devs, pair, block, leaf, dim, recv_ref, low_ref, high_ref, pts_ref, exch_ref, pos_ref, rolled, chg, pos_s, sem):
    half = pair // 2
    rows = pts_ref.shape[0]
    leaves = rows // leaf
    line = leaf + leaf // 2
    table = jnp.concatenate(
        [recv_ref[d * block + pair + half : d * block + pair + half + 1, :] for d in range(devs)], axis=0
    )
    pos_ref[...] = table.astype(jnp.int32)
    copy = pltpu.make_async_copy(pos_ref, pos_s, sem)
    copy.start()
    exch_ref[rows // 2 :, :] = table
    for d in range(devs):
        part = recv_ref[d * block + pair : d * block + pair + half, :]
        rolled[d * half : (d + 1) * half, :] = jnp.concatenate([part[:, dim:], part[:, :dim]], axis=1)
    copy.wait()

    def per_source(d, carry):
        for j in range(pair):
            p = pos_s[d, j]
            chg[pl.ds(p, 1), :] = recv_ref[pl.ds(d * block + j, 1), :]
            if j < half:
                pts_ref[pl.ds(p, 1), :] = recv_ref[pl.ds(d * block + pair + j, 1), :]
            else:
                pts_ref[pl.ds(p, 1), :] = rolled[pl.ds(d * half + j - half, 1), :]
        return carry

    lax.fori_loop(0, devs, per_source, 0)
    for g in range(leaves):
        packed = pack(pts_ref[g * leaf : (g + 1) * leaf, :], dim)
        ref, at = (low_ref, g * line) if g < leaves // 2 else (high_ref, (g - leaves // 2) * line)
        ref[at : at + leaf, :] = chg[g * leaf : (g + 1) * leaf, :]
        ref[at + leaf : at + line, :] = packed
        exch_ref[g * (leaf // 2) : (g + 1) * (leaf // 2), :] = packed


def skeleton_kernel(leaf, dim, low_ref, high_ref, pts_ref, interp_ref, skel_ref, far_ref, stmp):
    leaves, skel = skel_ref.shape
    line = leaf + leaf // 2
    fline = skel + skel // 2


    def gather(g, carry):
        for n in range(skel):
            stmp[pl.ds(g * skel + n, 1), :] = pts_ref[pl.ds(g * leaf + skel_ref[g, n], 1), :]
        return carry

    lax.fori_loop(0, leaves, gather, 0)
    for g in range(leaves):
        hi, lo = split(interp_ref[g * leaf : (g + 1) * leaf, :])
        ref, at = (low_ref, g * line) if g < leaves // 2 else (high_ref, (g - leaves // 2) * line)
        charge = charge_side(ref[at : at + leaf, :])
        far_ref[g * fline : g * fline + skel, :] = fold(tn_dot(hi, charge) + tn_dot(lo, charge))
        far_ref[g * fline + skel : (g + 1) * fline, :] = pack(stmp[g * skel : (g + 1) * skel, :], dim)


def far_kernel(skel, scale, n_inner, blocks, far_rows_ref, own_hbm, interp_hbm, *rest):
    hbm, (out_ref, src, chg, tgt), bufs, sems = rest[:blocks], rest[blocks : blocks + 4], rest[blocks + 4 : -1], rest[-1]
    own, *refs, interp = bufs
    copies = start_loads([own_hbm, *hbm, interp_hbm], bufs, sems)
    leaves, fars = far_rows_ref.shape
    leaf = interp_hbm.shape[0] // leaves
    fline = skel + skel // 2
    outer = lax.axis_index("outer")
    copies[0].wait()
    load_points(own, fline, skel, 0, tgt, scale, True)
    for b in range(blocks):
        copies[b + 1].wait()
        load_points(refs[b], fline, skel, b * leaves, src, scale, False)
        load_charges(refs[b], fline, b * leaves, chg)
    copies[-1].wait()

    for g in range(leaves):
        q = jnp.zeros((skel, LANES), F32)
        for k in range(0, fars, 2):
            ats = []
            for j in range(k, min(k + 2, fars)):
                device, local = div_mod(far_rows_ref[g, j], leaves)
                ats.append(((device // n_inner) ^ outer) * leaves - leaves + local)
            q = q + tile_product(
                tgt[g],
                jnp.concatenate([src[at] for at in ats], axis=0),
                jnp.concatenate([chg[at] for at in ats], axis=0),
            )
        qq = charge_side(q)
        hi, lo = split(interp[g * leaf : (g + 1) * leaf, :])
        out_ref[g * leaf : (g + 1) * leaf, :] = fold(
            jnp.dot(hi, qq, preferred_element_type=F32) + jnp.dot(lo, qq, preferred_element_type=F32)
        )


def target_kernel(leaf, scale, own_ref, theirs_ref, out_ref):
    leaves = own_ref.shape[0]
    out_ref[:leaves] = own_ref[...]
    load_points(theirs_ref.at[: leaves * leaf // 2], leaf // 2, 0, leaves, out_ref, scale, True)


CODE = 1024
GROUP = 4


def list_kernel(leaves, n_inner, near_ref, list_ref, count_ref):
    half = n_inner // 2
    cut = leaves // 2
    n_near = near_ref.shape[1]
    inner = lax.axis_index("inner")
    for row in range(4):
        count_ref[row] = 0

    def add(row, code):
        n = count_ref[row]
        list_ref[row, n] = code
        count_ref[row] = n + 1

    def entry(e, carry):
        row, k = div_mod(e, n_near)
        device, local = div_mod(near_ref[row, k], leaves)
        away = (device & (n_inner - 1)) ^ inner
        last = away == half - 1
        high = local >= cut
        theirs = row >= leaves
        which = jnp.where(last, jnp.where(high, 3, 2), jnp.where(theirs, 1, 0))
        source = jnp.where(last, jnp.where(high, local - cut, local), away * leaves + local)

        @pl.when((away < half) & ((away != 0) | theirs))
        def _():
            add(which, row * CODE + source)

        return carry

    lax.fori_loop(0, 2 * leaves * n_near, entry, 0)
    for row in range(4):
        for _ in range(GROUP - 1):

            @pl.when(count_ref[row] % GROUP != 0)
            def _():
                add(row, (leaves if row == 0 else 2 * leaves) * CODE)


def start_loads(hbm_refs, bufs, sems):
    copies = [pltpu.make_async_copy(a, b, sems.at[i]) for i, (a, b) in enumerate(zip(hbm_refs, bufs))]
    for copy in copies:
        copy.start()
    return copies


def load_sources(leaf, scale, refs, src, chg, at=0, copies=None):
    line = leaf + leaf // 2
    for i, ref in enumerate(refs):
        if copies:
            copies[i].wait()
        load_points(ref, line, leaf, at, src, scale, False)
        load_charges(ref, line, at, chg)
        at += ref.shape[0] // line


def leaf_rows(t, c, leaf, step):
    return pl.ds(pl.multiple_of(t * leaf + c, step), step)


def self_kernel(leaf, scale, own_ref, low_ref, high_ref, acc_ref, src, chg, tgt):
    leaves = src.shape[0]
    load_sources(leaf, scale, (low_ref, high_ref), src, chg)
    load_points(own_ref.at[: leaves * leaf // 2], leaf // 2, 0, 0, tgt, scale, True)
    step = leaf // 2

    def entry(e, carry):
        for t in (2 * e, 2 * e + 1):
            for c in range(0, leaf, step):
                acc_ref[leaf_rows(t, c, leaf, step), :] = tile_product(
                    tgt[t, c : c + step, :], src[t], chg[t]
                )
        return carry

    lax.fori_loop(0, leaves // 2, entry, 0)


def add_listed(leaf, row, list_ref, count_ref, tgt, src, chg, acc):
    step = leaf // 2

    def entry(e, carry):
        for u in range(GROUP):
            t, at = div_mod(list_ref[row, e * GROUP + u], CODE)
            x = jnp.minimum(t, tgt.shape[0] - 1)
            for c in range(0, leaf, step):
                acc[leaf_rows(t, c, leaf, step), :] += tile_product(
                    tgt[x, c : c + step, :], src[at], chg[at]
                )
        return carry

    lax.fori_loop(0, lax.shift_right_logical(count_ref[row], jnp.int32(GROUP.bit_length() - 1)), entry, 0)


def own_near_kernel(leaf, scale, list_ref, count_ref, tgt_ref, src_ref, chg_ref, *rest):
    n = (len(rest) - 4) // 2
    sources, (acc_ref, src, chg), bufs, sems = rest[:n], rest[n : n + 3], rest[n + 3 : -1], rest[-1]
    copies = start_loads(sources, bufs, sems)
    leaves = src_ref.shape[0]
    src[:leaves] = src_ref[...]
    chg[:leaves] = chg_ref[...]
    acc_ref[...] = jnp.zeros_like(acc_ref)
    load_sources(leaf, scale, bufs, src, chg, leaves, copies)
    add_listed(leaf, 0, list_ref, count_ref, tgt_ref, src, chg, acc_ref)


def near_kernel(leaf, scale, list_ref, count_ref, tgt_ref, src_ref, chg_ref, low_hbm, own_ref, acc_ref, src, chg, low, sems):
    rows = own_ref.shape[0] - leaf
    copies = start_loads([low_hbm], [low], sems)
    acc_ref[:rows, :] = own_ref[:rows, :]
    acc_ref[rows:, :] = jnp.zeros((acc_ref.shape[0] - rows, LANES), F32)
    add_listed(leaf, 1, list_ref, count_ref, tgt_ref, src_ref, chg_ref, acc_ref)
    load_sources(leaf, scale, (low,), src, chg, 0, copies)
    add_listed(leaf, 2, list_ref, count_ref, tgt_ref, src, chg, acc_ref)


def last_kernel(devs, pair, leaf, scale, list_ref, count_ref, pos_ref, tgt_ref, piece_hbm, old_ref, self_ref, far_ref, theirs_hbm, out_ref, acc, src, chg, opos_v, opos_s, sem, held, opos_f, sems):
    rows = far_ref.shape[0]
    table = theirs_hbm.at[pl.ds(rows // 2, devs), :]
    copies = start_loads([piece_hbm, table], [held, opos_f], sems)
    acc[:rows, :] = old_ref[:rows, :] + (self_ref[...] + far_ref[...])
    acc[rows:, :] = old_ref[rows:, :]
    copies[1].wait()
    opos_v[...] = opos_f[...].astype(jnp.int32)
    copy = pltpu.make_async_copy(opos_v, opos_s, sem)
    copy.start()
    load_sources(leaf, scale, (held,), src, chg, 0, copies)
    add_listed(leaf, 3, list_ref, count_ref, tgt_ref, src, chg, acc)
    copy.wait()

    def per_source(d, carry):
        for j in range(pair):
            out_ref[pl.ds(d * 2 * pair + j, 1), :] = acc[pl.ds(pos_ref[d, j], 1), :]
            out_ref[pl.ds(d * 2 * pair + pair + j, 1), :] = acc[pl.ds(rows + opos_s[d, j], 1), :]
        return carry

    lax.fori_loop(0, devs, per_source, 0)


def final_kernel(pair, n_inner, ret_ref, code_ref, out_hbm, both, out, sems):
    devs = both.shape[0] // pair
    for d in range(devs):
        other = d ^ (n_inner // 2)
        both[d * pair : (d + 1) * pair, :] = (
            ret_ref[2 * d * pair : (2 * d + 1) * pair, :]
            + ret_ref[(2 * other + 1) * pair : (2 * other + 2) * pair, :]
        )

    parts = sems.shape[0]
    size = out.shape[0] // parts
    steps = size // LANES
    copies = []
    for p in range(parts):

        def step(line, carry):
            for lane in range(LANES):
                row = both[pl.ds(code_ref[line, lane], 1), :]
                out[pl.ds(line * LANES + lane, 1), :] = row
            return carry

        lax.fori_loop(p * steps, (p + 1) * steps, step, 0)
        rows = pl.ds(p * size, size)
        copies.append(pltpu.make_async_copy(out.at[rows, :], out_hbm.at[rows, :], sems.at[p]))
        copies[-1].start()
    for copy in copies:
        copy.wait()


def shards(points, charges, interp, order, near, far, skel):
    n_inner = lax.axis_size("inner")
    n_outer = lax.axis_size("outer")
    devs = n_inner * n_outer
    rows, dim = points.shape
    leaves, n_skel = skel.shape
    leaf = rows // leaves
    line = leaf + leaf // 2
    fline = n_skel + n_skel // 2
    pair = rows // devs
    block = pair + pair // 2 + 8
    scale = (4.0 / dim) * math.log2(math.e)
    outer = lax.axis_index("outer")
    inner = lax.axis_index("inner")
    me = outer * n_inner + inner
    half = n_inner // 2
    partner = outer * n_inner + (inner ^ half)

    def f32(*shape):
        return jax.ShapeDtypeStruct(shape, F32)

    def i32(*shape):
        return jax.ShapeDtypeStruct(shape, jnp.int32)

    def near_of(device):
        return lax.dynamic_slice_in_dim(near, device * leaves, leaves, 0)

    near_rows = jnp.concatenate([near_of(me), near_of(partner)], axis=0)
    far_rows = lax.dynamic_slice_in_dim(far, me * leaves, leaves, 0)

    send, code = call(
        functools.partial(send_kernel, devs, pair, block),
        [f32(devs * block, LANES), i32(rows // LANES, LANES)],
        (order.reshape(rows // LANES, LANES), points.T, charges),
        [HBM] * 3,
        [
            pltpu.VMEM((devs * block, LANES), F32),
            pltpu.VMEM((rows, LANES), F32),
            pltpu.VMEM((rows // LANES, LANES), jnp.int32),
            pltpu.VMEM((dim, rows), F32),
            pltpu.VMEM((rows, LANES), F32),
            pltpu.VMEM((rows // LANES, LANES), jnp.int32),
            pltpu.SMEM((rows // LANES, LANES), jnp.int32),
            pltpu.SemaphoreType.DMA,
            pltpu.SemaphoreType.DMA((3,)),
        ],
        room=60,
    )
    recv = lax.all_to_all(send.reshape(devs, block, LANES), JOINT, 0, 0, tiled=True)
    piece = leaves // 2 * line
    own_low, own_high, pts, exch, pos = call(
        functools.partial(place_kernel, devs, pair, block, leaf, dim),
        [f32(piece, LANES), f32(piece, LANES), f32(rows, LANES), f32(rows // 2 + devs, LANES), i32(devs, LANES)],
        (recv.reshape(devs * block, LANES),),
        [VMEM],
        [
            pltpu.VMEM((devs * pair // 2, LANES), F32),
            pltpu.VMEM((rows, LANES), F32),
            pltpu.SMEM((devs, LANES), jnp.int32),
            pltpu.SemaphoreType.DMA,
        ],
    )

    def swap(x, bit):
        return lax.ppermute(x, "inner", [(i, i ^ bit) for i in range(n_inner)])

    blocks = {0: (own_low, own_high)}
    for r in sorted(range(1, half), key=lambda r: (r.bit_count(), r)):
        down, up = r & -r, 1 << (r.bit_length() - 1)
        by_low = 0 if r == down else r ^ down
        by_high = 0 if r == up else r ^ up
        blocks[r] = (swap(blocks[by_low][0], r ^ by_low), swap(blocks[by_high][1], r ^ by_high))
    theirs = swap(exch, half)

    (far_own,) = call(
        functools.partial(skeleton_kernel, leaf, dim),
        [f32(leaves * fline, LANES)],
        (own_low, own_high, pts, interp, skel),
        [VMEM, VMEM, VMEM, VMEM, SMEM],
        [pltpu.VMEM((leaves * n_skel, LANES), F32)],
        flops=2 * rows * n_skel * 3 * 128,
    )
    held = {0: far_own}
    bit = n_outer // 2
    while bit:
        perm = [(o, o ^ bit) for o in range(n_outer)]
        got = {}
        for r, v in held.items():
            got[r ^ bit] = lax.ppermute(v, "outer", perm)
        held.update(got)
        bit //= 2

    lists, counts = call(
        functools.partial(list_kernel, leaves, n_inner),
        [i32(4, 2 * leaves * near.shape[1]), i32(4)],
        (near_rows,),
        [SMEM],
        out_specs=[SMEM, SMEM],
    )

    def tiles(count):
        return [
            pltpu.VMEM((count, leaf, 4 * dim), BF16),
            pltpu.VMEM((count, leaf, 2 * LANES), BF16),
        ]

    per_leaf = 2 * leaf * leaf * 256 * 3
    own_sum, own_src, own_chg, own_tgt = call(
        functools.partial(self_kernel, leaf, scale),
        [f32(rows, LANES)] + [jax.ShapeDtypeStruct((leaves, leaf, 4 * dim), BF16)] * 3,
        (exch, own_low, own_high),
        [VMEM] * 3,
        flops=leaves * per_leaf,
    )
    (targets,) = call(
        functools.partial(target_kernel, leaf, scale),
        [jax.ShapeDtypeStruct((2 * leaves, leaf, 4 * dim), BF16)],
        (own_tgt, theirs),
        [VMEM] * 2,
        flops=1 << 20,
    )
    sources = [piece for r in range(1, half - 1) for piece in blocks[r]]
    held_tiles = [jax.ShapeDtypeStruct(((half - 1) * leaves, leaf, 4 * dim), BF16)] * 2
    acc, src, chg = call(
        functools.partial(own_near_kernel, leaf, scale),
        [f32(rows + leaf, LANES)] + held_tiles,
        (lists, counts, own_tgt, own_src, own_chg, *sources),
        [SMEM, SMEM] + [VMEM] * 3 + [HBM] * len(sources),
        [pltpu.VMEM((piece, LANES), F32)] * len(sources) + [pltpu.SemaphoreType.DMA((len(sources),))],
        flops=(half - 2) * leaves * per_leaf,
    )
    (acc,) = call(
        functools.partial(near_kernel, leaf, scale),
        [f32(2 * rows + leaf, LANES)],
        (lists, counts, targets, src, chg, blocks[half - 1][0], acc),
        [SMEM, SMEM] + [VMEM] * 3 + [HBM, VMEM],
        tiles(leaves // 2) + [pltpu.VMEM((piece, LANES), F32), pltpu.SemaphoreType.DMA((1,))],
        flops=half * leaves * per_leaf,
    )
    others = [held[r] for r in range(1, n_outer)]
    n_blocks = len(others) * leaves
    (far_part,) = call(
        functools.partial(far_kernel, n_skel, scale, n_inner, len(others)),
        [f32(rows, LANES)],
        (far_rows, far_own, interp, *others),
        [SMEM] + [HBM] * (2 + len(others)),
        [
            pltpu.VMEM((n_blocks, n_skel, 4 * dim), BF16),
            pltpu.VMEM((n_blocks, n_skel, 2 * LANES), BF16),
            pltpu.VMEM((leaves, n_skel, 4 * dim), BF16),
        ]
        + [pltpu.VMEM((leaves * fline, LANES), F32)] * (1 + len(others))
        + [pltpu.VMEM(interp.shape, F32), pltpu.SemaphoreType.DMA((2 + len(others),))],
        flops=leaves * 8 * 2 * n_skel * n_skel * 256 * 3,
    )
    (out,) = call(
        functools.partial(last_kernel, devs, pair, leaf, scale),
        [f32(devs * 2 * pair, LANES)],
        (lists, counts, pos, targets, blocks[half - 1][1], acc, own_sum, far_part, theirs),
        [SMEM] * 3 + [VMEM, HBM] + [VMEM] * 3 + [HBM],
        [pltpu.VMEM((2 * rows + leaf, LANES), F32)]
        + tiles(leaves // 2)
        + [
            pltpu.VMEM((devs, LANES), jnp.int32),
            pltpu.SMEM((devs, LANES), jnp.int32),
            pltpu.SemaphoreType.DMA,
            pltpu.VMEM((piece, LANES), F32),
            pltpu.VMEM((devs, LANES), F32),
            pltpu.SemaphoreType.DMA((2,)),
        ],
        flops=2 * leaves * per_leaf,
    )
    returned = lax.all_to_all(out.reshape(devs, 2 * pair, LANES), JOINT, 0, 0, tiled=True)
    (final,) = call(
        functools.partial(final_kernel, pair, n_inner),
        [f32(rows, LANES)],
        (returned.reshape(devs * 2 * pair, LANES), code),
        [VMEM, SMEM],
        [pltpu.VMEM((rows, LANES), F32), pltpu.VMEM((rows, LANES), F32), pltpu.SemaphoreType.DMA((4,))],
        out_specs=[HBM],
    )
    return final


def solution(mesh):
    row = P(JOINT, None)
    in_specs = (row, row, row, P(JOINT), P(), P(), row)
    return jax.shard_map(shards, mesh=mesh, in_specs=in_specs, out_specs=row, check_vma=False)
```

```python
import functools
import math

import jax
import jax.numpy as jnp
from jax import lax
from jax.experimental import pallas as pl
from jax.experimental.pallas import tpu as pltpu
from jax.sharding import PartitionSpec as P


F32 = jnp.float32
BF16 = jnp.bfloat16
LANES = 128
JOINT = ("outer", "inner")
VMEM = pl.BlockSpec(memory_space=pltpu.VMEM)
SMEM = pl.BlockSpec(memory_space=pltpu.SMEM)
HBM = pl.BlockSpec(memory_space=pltpu.HBM)


def call(body, outs, args, in_specs, scratch=(), out_specs=None, flops=0, room=3):
    nbytes = sum(a.size * a.dtype.itemsize for a in (*args, *outs))
    held = sum(math.prod(s.shape) * jnp.dtype(s.dtype).itemsize for s in scratch if getattr(s, "memory_space", None) == pltpu.VMEM)
    limit = min(60 << 20, nbytes + held + (room << 20))
    return pl.pallas_call(
        body,
        out_shape=outs,
        in_specs=in_specs,
        out_specs=out_specs or [VMEM] * len(outs),
        scratch_shapes=list(scratch),
        compiler_params=pltpu.CompilerParams(vmem_limit_bytes=limit),
        cost_estimate=pl.CostEstimate(flops=flops, bytes_accessed=nbytes, transcendentals=0),
    )(*args)


def split(x):
    hi = x.astype(BF16)
    return hi, (x - hi.astype(F32)).astype(BF16)


def pack(rows, dim):
    half = rows.shape[0] // 2
    return jnp.concatenate([rows[:half, :dim], rows[half:, :dim]], axis=1)


def exponent_side(packed, dim, scale, is_target):
    lane = lax.broadcasted_iota(jnp.int32, packed.shape, 1)
    first = lane < dim
    turned = jnp.concatenate([packed[:, dim:], packed[:, :dim]], axis=1)
    at = dim + (0 if is_target else 3)
    ones = jnp.where((lane >= dim) & (lane < dim + 6), 1.0, 0.0)
    blocks = []
    for x in (jnp.where(first, packed, turned), jnp.where(first, turned, packed)):
        n = jnp.sum(x * x, axis=1, keepdims=True) * (-0.5 * scale)
        norms = jnp.where(lane == at, n, ones)
        for j in (1, 2):
            n = n - n.astype(BF16).astype(F32)
            norms = jnp.where(lane == at + j, n, norms)
        if is_target:
            x = x * (2.0 * scale)
        low = x - x.astype(BF16).astype(F32)
        if is_target:
            head, tail = jnp.where(first, x, low), jnp.where(first, x, norms)
        else:
            head, tail = x, jnp.where(first, low, norms)
        blocks.append(jnp.concatenate([head, tail], axis=1).astype(BF16))
    return blocks


def load_points(ref, pitch, skip, base, out, scale, is_target):
    count = ref.shape[0] // pitch
    size = out.shape[1] // 2
    step = size
    parts = size // step

    def body(i, carry):
        g, c = div_mod(i, parts)
        at = pl.multiple_of(g * pitch + skip + c * step, 8)
        blocks = exponent_side(ref[pl.ds(at, step), :], LANES // 2, scale, is_target)
        for j, value in enumerate(blocks):
            out[base + g, pl.ds(pl.multiple_of(j * size + c * step, step), step), :] = value
        return carry

    lax.fori_loop(0, count * parts, body, 0)


def load_charges(ref, pitch, base, out):
    count = ref.shape[0] // pitch
    step = 256
    parts = out.shape[1] // step

    def body(i, carry):
        g, c = div_mod(i, parts)
        at = pl.multiple_of(g * pitch + c * step, 8)
        hi, lo = split(ref[pl.ds(at, step), :])
        rows = pl.ds(pl.multiple_of(c * step, step), step)
        out[base + g, rows, :LANES] = hi
        out[base + g, rows, LANES:] = lo
        return carry

    lax.fori_loop(0, count * parts, body, 0)


def charge_side(c):
    hi, lo = split(c)
    return jnp.concatenate([hi, lo], axis=1)


def nt_dot(a, b):
    return lax.dot_general(a, b, (((1,), (1,)), ((), ())), preferred_element_type=F32)


def tn_dot(a, b):
    return lax.dot_general(a, b, (((0,), (0,)), ((), ())), preferred_element_type=F32)


def fold(p):
    half = p.shape[1] // 2
    return p[:, :half] + p[:, half:]


def tile_product(target, source, charge):
    k = jnp.exp2(nt_dot(target, source))
    hi, lo = split(k)
    return fold(
        jnp.dot(hi, charge, preferred_element_type=F32)
        + jnp.dot(lo, charge, preferred_element_type=F32)
    )


def div_mod(x, n):
    if n & (n - 1) == 0:
        return lax.shift_right_logical(x, jnp.int32(n.bit_length() - 1)), x & (n - 1)
    q = lax.div(x, jnp.int32(n))
    return q, x - q * n


def rows_loop(count, body):
    def step(line, carry):
        for lane in range(LANES):
            body(line * LANES + lane, line, lane)
        return carry

    lax.fori_loop(0, count // LANES, step, 0)


def send_kernel(devs, pair, block, order_hbm, pts_hbm, chg_hbm, send_ref, code_ref, ptmp, prow, order_ref, pts_ref, chg_ref, idx_v, idx_s, sem, sems):
    loads = [
        pltpu.make_async_copy(a, b, sems.at[i])
        for i, (a, b) in enumerate(((order_hbm, order_ref), (chg_hbm, chg_ref), (pts_hbm, pts_ref)))
    ]
    for load in loads:
        load.start()
    loads[0].wait()
    rows = chg_ref.shape[0]
    dim = pts_ref.shape[0]
    lines = rows // LANES
    dest, slot = div_mod(order_ref[...], rows)
    sub = lax.broadcasted_iota(jnp.int32, (devs, LANES), 0)
    hot = [jnp.where(dest[r : r + 1, :] == sub, 1.0, 0.0) for r in range(lines)]
    ki = lax.broadcasted_iota(jnp.int32, (LANES, 2 * LANES), 0)
    ji = lax.broadcasted_iota(jnp.int32, (LANES, 2 * LANES), 1)
    tri = jnp.where((ki < ji) | (ji >= LANES), 1.0, 0.0).astype(BF16)
    pre = jnp.dot(jnp.concatenate([h.astype(BF16) for h in hot], axis=0), tri, preferred_element_type=F32)
    base = jnp.zeros((devs, LANES), F32)
    ranks = []
    for r in range(lines):
        part = pre[r * devs : (r + 1) * devs]
        ranks.append(jnp.sum(hot[r] * (part[:, :LANES] + base), axis=0, keepdims=True))
        base = base + part[:, LANES:]
    rank_f = jnp.concatenate(ranks, axis=0)
    rank = rank_f.astype(jnp.int32)
    idx_v[...] = dest * block + rank
    copy = pltpu.make_async_copy(idx_v, idx_s, sem)
    copy.start()
    code_ref[...] = dest * pair + rank
    psub = lax.broadcasted_iota(jnp.int32, (pair, LANES), 0)
    s_hi = lax.shift_right_logical(slot, 8).astype(F32)
    s_lo = (slot & 255).astype(F32)
    left, right = [], []
    for r in range(lines):
        left.append(
            jnp.concatenate([hot[r] * s_hi[r : r + 1, :], hot[r] * s_lo[r : r + 1, :]], axis=0).astype(BF16)
        )
        right.append(jnp.where(rank[r : r + 1, :] == psub, 1.0, 0.0).astype(BF16))
    both = nt_dot(jnp.concatenate(left, axis=1), jnp.concatenate(right, axis=1))
    table = both[:devs] * 256.0 + both[devs:]
    if pair < LANES:
        table = jnp.concatenate([table, jnp.zeros((devs, LANES - pair), F32)], axis=1)
    loads[2].wait()
    for c in range(0, rows, 256):
        prow[c : c + 256, :dim] = pts_ref[:, c : c + 256].T
    loads[1].wait()
    copy.wait()

    def move(n, line, lane):
        j = idx_s[line, lane]
        send_ref[pl.ds(j, 1), :] = chg_ref[pl.ds(n, 1), :]
        ptmp[pl.ds(j, 1), :] = prow[pl.ds(n, 1), :]

    rows_loop(rows, move)
    half = pair // 2
    for d in range(devs):
        send_ref[d * block + pair : d * block + pair + half, :] = pack(
            ptmp[d * block : d * block + pair, :], dim
        )
        send_ref[d * block + pair + half : (d + 1) * block, :] = jnp.broadcast_to(
            table[d : d + 1, :], (block - pair - half, LANES)
        )


def place_kernel(devs, pair, block, leaf, dim, recv_ref, low_ref, high_ref, pts_ref, exch_ref, pos_ref, rolled, chg, pos_s, sem):
    half = pair // 2
    rows = pts_ref.shape[0]
    leaves = rows // leaf
    line = leaf + leaf // 2
    table = jnp.concatenate(
        [recv_ref[d * block + pair + half : d * block + pair + half + 1, :] for d in range(devs)], axis=0
    )
    pos_ref[...] = table.astype(jnp.int32)
    copy = pltpu.make_async_copy(pos_ref, pos_s, sem)
    copy.start()
    exch_ref[rows // 2 :, :] = table
    for d in range(devs):
        part = recv_ref[d * block + pair : d * block + pair + half, :]
        rolled[d * half : (d + 1) * half, :] = jnp.concatenate([part[:, dim:], part[:, :dim]], axis=1)
    copy.wait()

    def per_source(d, carry):
        for j in range(pair):
            p = pos_s[d, j]
            chg[pl.ds(p, 1), :] = recv_ref[pl.ds(d * block + j, 1), :]
            if j < half:
                pts_ref[pl.ds(p, 1), :] = recv_ref[pl.ds(d * block + pair + j, 1), :]
            else:
                pts_ref[pl.ds(p, 1), :] = rolled[pl.ds(d * half + j - half, 1), :]
        return carry

    lax.fori_loop(0, devs, per_source, 0)
    for g in range(leaves):
        packed = pack(pts_ref[g * leaf : (g + 1) * leaf, :], dim)
        ref, at = (low_ref, g * line) if g < leaves // 2 else (high_ref, (g - leaves // 2) * line)
        ref[at : at + leaf, :] = chg[g * leaf : (g + 1) * leaf, :]
        ref[at + leaf : at + line, :] = packed
        exch_ref[g * (leaf // 2) : (g + 1) * (leaf // 2), :] = packed


def skeleton_kernel(leaf, dim, low_ref, high_ref, pts_ref, interp_ref, skel_ref, far_ref, stmp):
    leaves, skel = skel_ref.shape
    line = leaf + leaf // 2
    fline = skel + skel // 2


    def gather(g, carry):
        for n in range(skel):
            stmp[pl.ds(g * skel + n, 1), :] = pts_ref[pl.ds(g * leaf + skel_ref[g, n], 1), :]
        return carry

    lax.fori_loop(0, leaves, gather, 0)
    for g in range(leaves):
        hi, lo = split(interp_ref[g * leaf : (g + 1) * leaf, :])
        ref, at = (low_ref, g * line) if g < leaves // 2 else (high_ref, (g - leaves // 2) * line)
        charge = charge_side(ref[at : at + leaf, :])
        far_ref[g * fline : g * fline + skel, :] = fold(tn_dot(hi, charge) + tn_dot(lo, charge))
        far_ref[g * fline + skel : (g + 1) * fline, :] = pack(stmp[g * skel : (g + 1) * skel, :], dim)


def far_kernel(skel, scale, n_inner, blocks, far_rows_ref, own_hbm, interp_hbm, *rest):
    hbm, (out_ref, src, chg, tgt), bufs, sems = rest[:blocks], rest[blocks : blocks + 4], rest[blocks + 4 : -1], rest[-1]
    own, *refs, interp = bufs
    copies = start_loads([own_hbm, *hbm, interp_hbm], bufs, sems)
    leaves, fars = far_rows_ref.shape
    leaf = interp_hbm.shape[0] // leaves
    fline = skel + skel // 2
    outer = lax.axis_index("outer")
    copies[0].wait()
    load_points(own, fline, skel, 0, tgt, scale, True)
    for b in range(blocks):
        copies[b + 1].wait()
        load_points(refs[b], fline, skel, b * leaves, src, scale, False)
        load_charges(refs[b], fline, b * leaves, chg)
    copies[-1].wait()

    for g in range(leaves):
        q = jnp.zeros((skel, LANES), F32)
        for k in range(0, fars, 2):
            ats = []
            for j in range(k, min(k + 2, fars)):
                device, local = div_mod(far_rows_ref[g, j], leaves)
                ats.append(((device // n_inner) ^ outer) * leaves - leaves + local)
            q = q + tile_product(
                tgt[g],
                jnp.concatenate([src[at] for at in ats], axis=0),
                jnp.concatenate([chg[at] for at in ats], axis=0),
            )
        qq = charge_side(q)
        hi, lo = split(interp[g * leaf : (g + 1) * leaf, :])
        out_ref[g * leaf : (g + 1) * leaf, :] = fold(
            jnp.dot(hi, qq, preferred_element_type=F32) + jnp.dot(lo, qq, preferred_element_type=F32)
        )


def target_kernel(leaf, scale, own_ref, theirs_ref, out_ref):
    leaves = own_ref.shape[0]
    out_ref[:leaves] = own_ref[...]
    load_points(theirs_ref.at[: leaves * leaf // 2], leaf // 2, 0, leaves, out_ref, scale, True)


CODE = 1024
GROUP = 4


def list_kernel(leaves, n_inner, near_ref, list_ref, count_ref):
    half = n_inner // 2
    cut = leaves // 2
    n_near = near_ref.shape[1]
    inner = lax.axis_index("inner")
    for row in range(4):
        count_ref[row] = 0

    def add(row, code):
        n = count_ref[row]
        list_ref[row, n] = code
        count_ref[row] = n + 1

    def entry(e, carry):
        row, k = div_mod(e, n_near)
        device, local = div_mod(near_ref[row, k], leaves)
        away = (device & (n_inner - 1)) ^ inner
        last = away == half - 1
        high = local >= cut
        theirs = row >= leaves
        which = jnp.where(last, jnp.where(high, 3, 2), jnp.where(theirs, 1, 0))
        source = jnp.where(last, jnp.where(high, local - cut, local), away * leaves + local)

        @pl.when((away < half) & ((away != 0) | theirs))
        def _():
            add(which, row * CODE + source)

        return carry

    lax.fori_loop(0, 2 * leaves * n_near, entry, 0)
    for row in range(4):
        for _ in range(GROUP - 1):

            @pl.when(count_ref[row] % GROUP != 0)
            def _():
                add(row, (leaves if row == 0 else 2 * leaves) * CODE)


def start_loads(hbm_refs, bufs, sems):
    copies = [pltpu.make_async_copy(a, b, sems.at[i]) for i, (a, b) in enumerate(zip(hbm_refs, bufs))]
    for copy in copies:
        copy.start()
    return copies


def load_sources(leaf, scale, refs, src, chg, at=0, copies=None):
    line = leaf + leaf // 2
    for i, ref in enumerate(refs):
        if copies:
            copies[i].wait()
        load_points(ref, line, leaf, at, src, scale, False)
        load_charges(ref, line, at, chg)
        at += ref.shape[0] // line


def leaf_rows(t, c, leaf, step):
    return pl.ds(pl.multiple_of(t * leaf + c, step), step)


def self_kernel(leaf, scale, own_ref, low_ref, high_ref, acc_ref, src, chg, tgt):
    leaves = src.shape[0]
    load_sources(leaf, scale, (low_ref, high_ref), src, chg)
    load_points(own_ref.at[: leaves * leaf // 2], leaf // 2, 0, 0, tgt, scale, True)
    step = leaf // 2

    def entry(e, carry):
        for t in (2 * e, 2 * e + 1):
            for c in range(0, leaf, step):
                acc_ref[leaf_rows(t, c, leaf, step), :] = tile_product(
                    tgt[t, c : c + step, :], src[t], chg[t]
                )
        return carry

    lax.fori_loop(0, leaves // 2, entry, 0)


def add_listed(leaf, row, list_ref, count_ref, tgt, src, chg, acc):
    step = leaf // 2

    def entry(e, carry):
        for u in range(GROUP):
            t, at = div_mod(list_ref[row, e * GROUP + u], CODE)
            x = jnp.minimum(t, tgt.shape[0] - 1)
            for c in range(0, leaf, step):
                acc[leaf_rows(t, c, leaf, step), :] += tile_product(
                    tgt[x, c : c + step, :], src[at], chg[at]
                )
        return carry

    lax.fori_loop(0, lax.shift_right_logical(count_ref[row], jnp.int32(GROUP.bit_length() - 1)), entry, 0)


def own_near_kernel(leaf, scale, list_ref, count_ref, tgt_ref, src_ref, chg_ref, self_ref, *rest):
    n = (len(rest) - 4) // 2
    sources, (acc_ref, src, chg), bufs, sems = rest[:n], rest[n : n + 3], rest[n + 3 : -1], rest[-1]
    copies = start_loads(sources, bufs, sems)
    leaves = src_ref.shape[0]
    src[:leaves] = src_ref[...]
    chg[:leaves] = chg_ref[...]
    acc_ref[: self_ref.shape[0], :] = self_ref[...]
    load_sources(leaf, scale, bufs, src, chg, leaves, copies)
    add_listed(leaf, 0, list_ref, count_ref, tgt_ref, src, chg, acc_ref)


def near_kernel(leaf, scale, list_ref, count_ref, tgt_ref, src_ref, chg_ref, low_hbm, own_ref, far_ref, acc_ref, src, chg, low, sems):
    rows = own_ref.shape[0] - leaf
    copies = start_loads([low_hbm], [low], sems)
    acc_ref[:rows, :] = own_ref[:rows, :] + far_ref[...]
    acc_ref[rows:, :] = jnp.zeros((acc_ref.shape[0] - rows, LANES), F32)
    add_listed(leaf, 1, list_ref, count_ref, tgt_ref, src_ref, chg_ref, acc_ref)
    load_sources(leaf, scale, (low,), src, chg, 0, copies)
    add_listed(leaf, 2, list_ref, count_ref, tgt_ref, src, chg, acc_ref)


def last_kernel(devs, pair, leaf, scale, list_ref, count_ref, pos_ref, tgt_ref, piece_hbm, old_ref, theirs_hbm, out_ref, acc, src, chg, opos_v, opos_s, sem, held, opos_f, sems):
    rows = (acc.shape[0] - leaf) // 2
    table = theirs_hbm.at[pl.ds(rows // 2, devs), :]
    copies = start_loads([piece_hbm, table], [held, opos_f], sems)
    acc[...] = old_ref[...]
    copies[1].wait()
    opos_v[...] = opos_f[...].astype(jnp.int32)
    copy = pltpu.make_async_copy(opos_v, opos_s, sem)
    copy.start()
    load_sources(leaf, scale, (held,), src, chg, 0, copies)
    add_listed(leaf, 3, list_ref, count_ref, tgt_ref, src, chg, acc)
    copy.wait()

    def per_source(d, carry):
        for j in range(pair):
            out_ref[pl.ds(d * 2 * pair + j, 1), :] = acc[pl.ds(pos_ref[d, j], 1), :]
            out_ref[pl.ds(d * 2 * pair + pair + j, 1), :] = acc[pl.ds(rows + opos_s[d, j], 1), :]
        return carry

    lax.fori_loop(0, devs, per_source, 0)


def final_kernel(pair, n_inner, ret_ref, code_ref, out_hbm, both, out, sems):
    devs = both.shape[0] // pair
    for d in range(devs):
        other = d ^ (n_inner // 2)
        both[d * pair : (d + 1) * pair, :] = (
            ret_ref[2 * d * pair : (2 * d + 1) * pair, :]
            + ret_ref[(2 * other + 1) * pair : (2 * other + 2) * pair, :]
        )

    parts = sems.shape[0]
    size = out.shape[0] // parts
    steps = size // LANES
    copies = []
    for p in range(parts):

        def step(line, carry):
            for lane in range(LANES):
                row = both[pl.ds(code_ref[line, lane], 1), :]
                out[pl.ds(line * LANES + lane, 1), :] = row
            return carry

        lax.fori_loop(p * steps, (p + 1) * steps, step, 0)
        rows = pl.ds(p * size, size)
        copies.append(pltpu.make_async_copy(out.at[rows, :], out_hbm.at[rows, :], sems.at[p]))
        copies[-1].start()
    for copy in copies:
        copy.wait()


def shards(points, charges, interp, order, near, far, skel):
    n_inner = lax.axis_size("inner")
    n_outer = lax.axis_size("outer")
    devs = n_inner * n_outer
    rows, dim = points.shape
    leaves, n_skel = skel.shape
    leaf = rows // leaves
    line = leaf + leaf // 2
    fline = n_skel + n_skel // 2
    pair = rows // devs
    block = pair + pair // 2 + 8
    scale = (4.0 / dim) * math.log2(math.e)
    outer = lax.axis_index("outer")
    inner = lax.axis_index("inner")
    me = outer * n_inner + inner
    half = n_inner // 2
    partner = outer * n_inner + (inner ^ half)

    def f32(*shape):
        return jax.ShapeDtypeStruct(shape, F32)

    def i32(*shape):
        return jax.ShapeDtypeStruct(shape, jnp.int32)

    def near_of(device):
        return lax.dynamic_slice_in_dim(near, device * leaves, leaves, 0)

    near_rows = jnp.concatenate([near_of(me), near_of(partner)], axis=0)
    far_rows = lax.dynamic_slice_in_dim(far, me * leaves, leaves, 0)

    send, code = call(
        functools.partial(send_kernel, devs, pair, block),
        [f32(devs * block, LANES), i32(rows // LANES, LANES)],
        (order.reshape(rows // LANES, LANES), points.T, charges),
        [HBM] * 3,
        [
            pltpu.VMEM((devs * block, LANES), F32),
            pltpu.VMEM((rows, LANES), F32),
            pltpu.VMEM((rows // LANES, LANES), jnp.int32),
            pltpu.VMEM((dim, rows), F32),
            pltpu.VMEM((rows, LANES), F32),
            pltpu.VMEM((rows // LANES, LANES), jnp.int32),
            pltpu.SMEM((rows // LANES, LANES), jnp.int32),
            pltpu.SemaphoreType.DMA,
            pltpu.SemaphoreType.DMA((3,)),
        ],
        room=60,
    )
    recv = lax.all_to_all(send.reshape(devs, block, LANES), JOINT, 0, 0, tiled=True)
    piece = leaves // 2 * line
    own_low, own_high, pts, exch, pos = call(
        functools.partial(place_kernel, devs, pair, block, leaf, dim),
        [f32(piece, LANES), f32(piece, LANES), f32(rows, LANES), f32(rows // 2 + devs, LANES), i32(devs, LANES)],
        (recv.reshape(devs * block, LANES),),
        [VMEM],
        [
            pltpu.VMEM((devs * pair // 2, LANES), F32),
            pltpu.VMEM((rows, LANES), F32),
            pltpu.SMEM((devs, LANES), jnp.int32),
            pltpu.SemaphoreType.DMA,
        ],
    )

    def swap(x, bit):
        return lax.ppermute(x, "inner", [(i, i ^ bit) for i in range(n_inner)])

    blocks = {0: (own_low, own_high)}
    for r in sorted(range(1, half), key=lambda r: (r.bit_count(), r)):
        down, up = r & -r, 1 << (r.bit_length() - 1)
        by_low = 0 if r == down else r ^ down
        by_high = 0 if r == up else r ^ up
        blocks[r] = (swap(blocks[by_low][0], r ^ by_low), swap(blocks[by_high][1], r ^ by_high))
    theirs = swap(exch, half)

    (far_own,) = call(
        functools.partial(skeleton_kernel, leaf, dim),
        [f32(leaves * fline, LANES)],
        (own_low, own_high, pts, interp, skel),
        [VMEM, VMEM, VMEM, VMEM, SMEM],
        [pltpu.VMEM((leaves * n_skel, LANES), F32)],
        flops=2 * rows * n_skel * 3 * 128,
    )
    held = {0: far_own}
    bit = n_outer // 2
    while bit:
        perm = [(o, o ^ bit) for o in range(n_outer)]
        got = {}
        for r, v in held.items():
            got[r ^ bit] = lax.ppermute(v, "outer", perm)
        held.update(got)
        bit //= 2

    lists, counts = call(
        functools.partial(list_kernel, leaves, n_inner),
        [i32(4, 2 * leaves * near.shape[1]), i32(4)],
        (near_rows,),
        [SMEM],
        out_specs=[SMEM, SMEM],
    )

    def tiles(count):
        return [
            pltpu.VMEM((count, leaf, 4 * dim), BF16),
            pltpu.VMEM((count, leaf, 2 * LANES), BF16),
        ]

    per_leaf = 2 * leaf * leaf * 256 * 3
    own_sum, own_src, own_chg, own_tgt = call(
        functools.partial(self_kernel, leaf, scale),
        [f32(rows, LANES)] + [jax.ShapeDtypeStruct((leaves, leaf, 4 * dim), BF16)] * 3,
        (exch, own_low, own_high),
        [VMEM] * 3,
        flops=leaves * per_leaf,
    )
    (targets,) = call(
        functools.partial(target_kernel, leaf, scale),
        [jax.ShapeDtypeStruct((2 * leaves, leaf, 4 * dim), BF16)],
        (own_tgt, theirs),
        [VMEM] * 2,
        flops=1 << 20,
    )
    others = [held[r] for r in range(1, n_outer)]
    n_blocks = len(others) * leaves
    (far_part,) = call(
        functools.partial(far_kernel, n_skel, scale, n_inner, len(others)),
        [f32(rows, LANES)],
        (far_rows, far_own, interp, *others),
        [SMEM] + [HBM] * (2 + len(others)),
        [
            pltpu.VMEM((n_blocks, n_skel, 4 * dim), BF16),
            pltpu.VMEM((n_blocks, n_skel, 2 * LANES), BF16),
            pltpu.VMEM((leaves, n_skel, 4 * dim), BF16),
        ]
        + [pltpu.VMEM((leaves * fline, LANES), F32)] * (1 + len(others))
        + [pltpu.VMEM(interp.shape, F32), pltpu.SemaphoreType.DMA((2 + len(others),))],
        flops=leaves * 8 * 2 * n_skel * n_skel * 256 * 3,
    )
    sources = [piece for r in range(1, half - 1) for piece in blocks[r]]
    held_tiles = [jax.ShapeDtypeStruct(((half - 1) * leaves, leaf, 4 * dim), BF16)] * 2
    acc, src, chg = call(
        functools.partial(own_near_kernel, leaf, scale),
        [f32(rows + leaf, LANES)] + held_tiles,
        (lists, counts, own_tgt, own_src, own_chg, own_sum, *sources),
        [SMEM, SMEM] + [VMEM] * 4 + [HBM] * len(sources),
        [pltpu.VMEM((piece, LANES), F32)] * len(sources) + [pltpu.SemaphoreType.DMA((len(sources),))],
        flops=(half - 2) * leaves * per_leaf,
    )
    (acc,) = call(
        functools.partial(near_kernel, leaf, scale),
        [f32(2 * rows + leaf, LANES)],
        (lists, counts, targets, src, chg, blocks[half - 1][0], acc, far_part),
        [SMEM, SMEM] + [VMEM] * 3 + [HBM, VMEM, VMEM],
        tiles(leaves // 2) + [pltpu.VMEM((piece, LANES), F32), pltpu.SemaphoreType.DMA((1,))],
        flops=half * leaves * per_leaf,
    )
    (out,) = call(
        functools.partial(last_kernel, devs, pair, leaf, scale),
        [f32(devs * 2 * pair, LANES)],
        (lists, counts, pos, targets, blocks[half - 1][1], acc, theirs),
        [SMEM] * 3 + [VMEM, HBM, VMEM, HBM],
        [pltpu.VMEM((2 * rows + leaf, LANES), F32)]
        + tiles(leaves // 2)
        + [
            pltpu.VMEM((devs, LANES), jnp.int32),
            pltpu.SMEM((devs, LANES), jnp.int32),
            pltpu.SemaphoreType.DMA,
            pltpu.VMEM((piece, LANES), F32),
            pltpu.VMEM((devs, LANES), F32),
            pltpu.SemaphoreType.DMA((2,)),
        ],
        flops=2 * leaves * per_leaf,
    )
    returned = lax.all_to_all(out.reshape(devs, 2 * pair, LANES), JOINT, 0, 0, tiled=True)
    (final,) = call(
        functools.partial(final_kernel, pair, n_inner),
        [f32(rows, LANES)],
        (returned.reshape(devs * 2 * pair, LANES), code),
        [VMEM, SMEM],
        [pltpu.VMEM((rows, LANES), F32), pltpu.VMEM((rows, LANES), F32), pltpu.SemaphoreType.DMA((4,))],
        out_specs=[HBM],
    )
    return final


def solution(mesh):
    row = P(JOINT, None)
    in_specs = (row, row, row, P(JOINT), P(), P(), row)
    return jax.shard_map(shards, mesh=mesh, in_specs=in_specs, out_specs=row, check_vma=False)
```
